32 devices in a mesh: seq: 16 (over z, y, x), rep: 2 (over core).
Axes of the slice: x: 2, y: 2, z: 4, core: 2. Of those that a mesh axis runs over, the one named last changes fastest.
Arguments:
- tokens: bfloat16 [4, 48, 180, 768], P('rep', 'seq'), may hold values from -6 to 6
- cotangent: bfloat16 [4, 48, 180, 768], P('rep', 'seq'), may hold values from -6 to 6
- in_weight: bfloat16 [2, 8, 96, 96], replicated, may hold values from -0.21875 to 0.21875
- in_bias: float32 [2, 768], replicated, may hold values from -0.6 to 0.6
- out_weight: bfloat16 [2, 8, 96, 96], replicated, may hold values from -0.21875 to 0.21875
- out_bias: float32 [2, 768], replicated, may hold values from -0.12 to 0.12
Outputs:
- mixed_out: bfloat16 [4, 48, 180, 768], P('rep', 'seq')
- tokens_grad: bfloat16 [4, 48, 180, 768], P('rep', 'seq')
- in_weight_grad: float32 [2, 8, 96, 96], replicated
- in_bias_grad: float32 [2, 768], replicated
- out_weight_grad: float32 [2, 8, 96, 96], replicated
- out_bias_grad: float32 [2, 768], replicated
The draws below stay inside these ranges and needn't reach their ends.
All inputs are finite; a program needn't handle non-finite values.
Results may differ from the reference program's by a relative error of at most 0.0094.
Values may be sent and summed in bfloat16 or wider, within the bound.
A program may use at most 64 MiB of HBM per device.

```python
import math
import jax
import jax.numpy as jnp
from jax import lax

D = 768
BLOCKS = 8
BLOCK = 96
COLS = 180
MODES = 64
ROWS = 48
BATCH = 4


def shard_levels(key, extent, cuts, low, largest):
    def one(axis_at, shards_of):
        heights = jax.random.uniform(jax.random.fold_in(jax.random.fold_in(key, 6), axis_at), (shards_of,), jnp.float32, low / len(cuts), largest / len(cuts))
        return jnp.repeat(jnp.exp(heights), extent[axis_at] // shards_of).reshape((-1,) + (1,) * (len(extent) - axis_at - 1))

    factor_of = one(*cuts[0])
    for cut in cuts[1:]:
        factor_of = factor_of * one(*cut)
    return factor_of


def scatter_about(key, dims, width, limit, pieces=(), kind=jnp.bfloat16):
    drawn = width * jax.random.normal(key, dims, jnp.float32)
    if pieces:
        drawn = drawn * shard_levels(key, dims, pieces, -0.22, 0.18)
    return jnp.clip(drawn, -limit, limit).astype(kind)


def setup_inputs(seed: int = 0) -> dict:
    splits = jax.random.split(jax.random.key(seed), 7)
    tokens = scatter_about(splits[0], (BATCH, ROWS, COLS, D), 1.0, 6.0, ((0, 2), (1, 16)))
    cotangent = scatter_about(splits[1], (BATCH, ROWS, COLS, D), 1.0, 6.0, ((0, 2), (1, 16)))
    in_weight = scatter_about(splits[2], (2, BLOCKS, BLOCK, BLOCK), (8 * BLOCK) ** -0.5, 0.21875)
    in_bias = scatter_about(splits[3], (2, D), 0.1, 0.6, (), jnp.float32)
    out_weight = scatter_about(splits[4], (2, BLOCKS, BLOCK, BLOCK), (8 * BLOCK) ** -0.5, 0.21875)
    out_bias = scatter_about(splits[5], (2, D), 0.02, 0.12, (), jnp.float32)
    return {"tokens": tokens, "cotangent": cotangent, "in_weight": in_weight, "in_bias": in_bias, "out_weight": out_weight, "out_bias": out_bias}


def widen(operand):
    return operand.astype(jnp.float32)

def grid_tables(length, modes):
    position = jnp.arange(length, dtype=jnp.int32)
    frequency = jnp.arange(modes, dtype=jnp.int32)
    residue = position[:, None] * frequency[None, :] % length
    angles = residue.astype(jnp.float32) * (2.0 * math.pi / length)
    factor = 1.0 / math.sqrt(length)
    cosine_table = (jnp.cos(angles) * factor).astype(jnp.bfloat16)
    sine_table = (jnp.sin(angles) * factor).astype(jnp.bfloat16)
    return (cosine_table, sine_table)

def column_tables(grid_width, modes):
    cosine_table, sine_table = grid_tables(grid_width, modes)
    forward = jnp.stack([cosine_table, -sine_table], axis=2)
    doubling = jnp.where(jnp.arange(modes) == 0, 1.0, 2.0).astype(jnp.bfloat16)[:, None]
    inverse = jnp.stack([cosine_table.T * doubling, -(sine_table.T * doubling)], axis=1)
    return (forward, inverse)

def row_table(length):
    cosine_table, sine_table = grid_tables(length, length)
    upper_rows = jnp.stack([cosine_table, sine_table], axis=2)
    lower_rows = jnp.stack([-sine_table, cosine_table], axis=2)
    return jnp.stack([upper_rows, lower_rows], axis=1)

def block_weights(weight):
    real_part, imag_part = (weight[0], weight[1])
    upper_half = jnp.stack([real_part, imag_part], axis=2)
    lower_half = jnp.stack([-imag_part, real_part], axis=2)
    return jnp.stack([upper_half, lower_half], axis=1)

def fold_blocks(blockwise):
    real_part = blockwise[:, 0, :, 0, :] + blockwise[:, 1, :, 1, :]
    imag_part = blockwise[:, 0, :, 1, :] - blockwise[:, 1, :, 0, :]
    return jnp.stack([real_part, imag_part])

def reference(tokens, cotangent, in_weight, in_bias, out_weight, out_bias):
    column_forward, column_inverse = column_tables(COLS, MODES)
    row_matrix = row_table(ROWS)
    weights_in = block_weights(in_weight)
    weights_out = block_weights(out_weight)
    bias_in = in_bias.reshape(2, BLOCKS, BLOCK)
    bias_out = out_bias.reshape(2, BLOCKS, BLOCK)
    mode_count = ROWS * MODES

    def one_sample(pair):
        sample_tokens, sample_cotangent = pair
        spec_rows = jnp.einsum('hwd,wkc->hkcd', widen(sample_tokens), widen(column_forward)).astype(jnp.bfloat16)
        spectrum = jnp.einsum('qehc,hkcd->qked', widen(row_matrix), widen(spec_rows)).astype(jnp.bfloat16)
        flat_modes = spectrum.reshape(mode_count, 2, BLOCKS, BLOCK)
        hidden_pre = jnp.einsum('mcbi,bciej->mebj', widen(flat_modes), widen(weights_in)) + bias_in
        hidden = jax.nn.gelu(hidden_pre).astype(jnp.bfloat16)
        spectrum_out = (jnp.einsum('mcbi,bciej->mebj', widen(hidden), widen(weights_out)) + bias_out).astype(jnp.bfloat16)
        back_rows = jnp.einsum('qehc,qked->hkcd', widen(row_matrix), widen(spectrum_out.reshape(ROWS, MODES, 2, D))).astype(jnp.bfloat16)
        mixed = (widen(sample_tokens) + jnp.einsum('hkcd,kcw->hwd', widen(back_rows), widen(column_inverse))).astype(jnp.bfloat16)
        cot_rows = jnp.einsum('hwd,kcw->hkcd', widen(sample_cotangent), widen(column_inverse)).astype(jnp.bfloat16)
        incoming = jnp.einsum('qehc,hkcd->qked', widen(row_matrix), widen(cot_rows)).astype(jnp.bfloat16)
        incoming = incoming.reshape(mode_count, 2, BLOCKS, BLOCK)
        out_bias_part = lax.optimization_barrier(jnp.sum(widen(incoming), axis=0)).reshape(2, D)
        out_weight_part = fold_blocks(jnp.einsum('mcbi,mebj->bciej', widen(hidden), widen(incoming)))
        hidden_grad = jnp.einsum('mebj,bciej->mcbi', widen(incoming), widen(weights_out))
        pre_grad = jax.vjp(jax.nn.gelu, hidden_pre)[1](hidden_grad)[0].astype(jnp.bfloat16)
        in_bias_part = lax.optimization_barrier(jnp.sum(widen(pre_grad), axis=0)).reshape(2, D)
        in_weight_part = fold_blocks(jnp.einsum('mcbi,mebj->bciej', widen(flat_modes), widen(pre_grad)))
        spectrum_grad = jnp.einsum('mebj,bciej->mcbi', widen(pre_grad), widen(weights_in)).astype(jnp.bfloat16)
        rows_grad = jnp.einsum('qehc,qked->hkcd', widen(row_matrix), widen(spectrum_grad.reshape(ROWS, MODES, 2, D))).astype(jnp.bfloat16)
        grad_tokens = (widen(sample_cotangent) + jnp.einsum('hkcd,wkc->hwd', widen(rows_grad), widen(column_forward))).astype(jnp.bfloat16)
        return (mixed, grad_tokens, in_weight_part, in_bias_part, out_weight_part, out_bias_part)
    outcome = lax.map(one_sample, (tokens, cotangent))
    return (outcome[0], outcome[1], lax.optimization_barrier(jnp.sum(outcome[2], axis=0)) / BATCH, lax.optimization_barrier(jnp.sum(outcome[3], axis=0)) / BATCH, lax.optimization_barrier(jnp.sum(outcome[4], axis=0)) / BATCH, lax.optimization_barrier(jnp.sum(outcome[5], axis=0)) / BATCH)
```

```python
import functools
import math

import jax
import jax.numpy as jnp
import ml_dtypes
import numpy as np
from jax import lax
from jax.experimental import pallas as pl
from jax.experimental.pallas import tpu as pltpu
from jax.sharding import PartitionSpec as P

BLOCKS = 8
BLOCK = 96
MODES = 64


def grid_tables(length, modes):
    position = jnp.arange(length, dtype=jnp.int32)
    frequency = jnp.arange(modes, dtype=jnp.int32)
    residue = position[:, None] * frequency[None, :] % length
    angles = residue.astype(jnp.float32) * (2.0 * math.pi / length)
    factor = 1.0 / math.sqrt(length)
    cosine_table = (jnp.cos(angles) * factor).astype(jnp.bfloat16)
    sine_table = (jnp.sin(angles) * factor).astype(jnp.bfloat16)
    return (cosine_table, sine_table)


def column_tables(grid_width, modes):
    cosine_table, sine_table = grid_tables(grid_width, modes)
    forward = jnp.stack([cosine_table, -sine_table], axis=2)
    doubling = jnp.where(jnp.arange(modes) == 0, 1.0, 2.0).astype(jnp.bfloat16)[:, None]
    inverse = jnp.stack([cosine_table.T * doubling, -(sine_table.T * doubling)], axis=1)
    return (forward, inverse)


def row_table(length):
    cosine_table, sine_table = grid_tables(length, length)
    upper_rows = jnp.stack([cosine_table, sine_table], axis=2)
    lower_rows = jnp.stack([-sine_table, cosine_table], axis=2)
    return jnp.stack([upper_rows, lower_rows], axis=1)


def block_weights(weight):
    real_part, imag_part = (weight[0], weight[1])
    upper_half = jnp.stack([real_part, imag_part], axis=2)
    lower_half = jnp.stack([-imag_part, real_part], axis=2)
    return jnp.stack([upper_half, lower_half], axis=1)


def fold_blocks(blockwise):
    real_part = blockwise[:, 0, :, 0, :] + blockwise[:, 1, :, 1, :]
    imag_part = blockwise[:, 0, :, 1, :] - blockwise[:, 1, :, 0, :]
    return jnp.stack([real_part, imag_part])


def mix_forward(spectrum, weights_in, weights_out, bias_in, bias_out):
    mode_count = spectrum.shape[0] * spectrum.shape[1] * spectrum.shape[2]
    flat_modes = spectrum.reshape(mode_count, 2, BLOCKS, BLOCK)
    hidden_pre = (
        jnp.einsum("mcbi,bciej->mebj", flat_modes, weights_in, preferred_element_type=jnp.float32)
        + bias_in
    )
    hidden = jax.nn.gelu(hidden_pre).astype(jnp.bfloat16)
    spectrum_out = (
        jnp.einsum("mcbi,bciej->mebj", hidden, weights_out, preferred_element_type=jnp.float32)
        + bias_out
    )
    return (
        flat_modes,
        hidden_pre,
        hidden,
        spectrum_out.astype(jnp.bfloat16).reshape(spectrum.shape),
    )


def mix_backward(flat_modes, hidden_pre, hidden, incoming, weights_in, weights_out):
    incoming_flat = incoming.reshape(flat_modes.shape)
    out_bias_part = jnp.sum(incoming_flat.astype(jnp.float32), axis=0).reshape(2, -1)
    out_weight_part = fold_blocks(
        jnp.einsum("mcbi,mebj->bciej", hidden, incoming_flat, preferred_element_type=jnp.float32)
    )
    hidden_grad = jnp.einsum(
        "mebj,bciej->mcbi", incoming_flat, weights_out, preferred_element_type=jnp.float32
    )
    pre_grad = jax.vjp(jax.nn.gelu, hidden_pre)[1](hidden_grad)[0].astype(jnp.bfloat16)
    in_bias_part = jnp.sum(pre_grad.astype(jnp.float32), axis=0).reshape(2, -1)
    in_weight_part = fold_blocks(
        jnp.einsum("mcbi,mebj->bciej", flat_modes, pre_grad, preferred_element_type=jnp.float32)
    )
    spectrum_grad = jnp.einsum(
        "mebj,bciej->mcbi", pre_grad, weights_in, preferred_element_type=jnp.float32
    )
    spectrum_grad = spectrum_grad.astype(jnp.bfloat16).reshape(incoming.shape)
    return (spectrum_grad, (in_weight_part, in_bias_part, out_weight_part, out_bias_part))


def shards_plain(tokens, cotangent, in_weight, in_bias, out_weight, out_bias):
    samples, row_count, grid_width, channels = tokens.shape
    length = row_count * lax.axis_size("seq")
    column_forward, column_inverse = column_tables(grid_width, MODES)
    row_matrix = row_table(length)
    weights_in = block_weights(in_weight)
    weights_out = block_weights(out_weight)
    bias_in = in_bias.reshape(2, BLOCKS, BLOCK)
    bias_out = out_bias.reshape(2, BLOCKS, BLOCK)

    def along_rows(section):
        return jnp.einsum(
            "qehc,shkcd->sqked", row_matrix, section, preferred_element_type=jnp.float32
        ).astype(jnp.bfloat16)

    def back_rows(section):
        return jnp.einsum(
            "qehc,sqked->shkcd", row_matrix, section, preferred_element_type=jnp.float32
        ).astype(jnp.bfloat16)

    spec_rows = jnp.einsum(
        "shwd,wkc->shkcd", tokens, column_forward, preferred_element_type=jnp.float32
    ).astype(jnp.bfloat16)
    spectrum = along_rows(lax.all_to_all(spec_rows, "seq", split_axis=2, concat_axis=1, tiled=True))
    flat_modes, hidden_pre, hidden, spectrum_out = mix_forward(
        spectrum, weights_in, weights_out, bias_in, bias_out
    )
    mixed_grid = jnp.einsum(
        "shkcd,kcw->shwd",
        lax.all_to_all(back_rows(spectrum_out), "seq", split_axis=1, concat_axis=2, tiled=True),
        column_inverse,
        preferred_element_type=jnp.float32,
    )
    cot_rows = jnp.einsum(
        "shwd,kcw->shkcd", cotangent, column_inverse, preferred_element_type=jnp.float32
    ).astype(jnp.bfloat16)
    incoming = along_rows(lax.all_to_all(cot_rows, "seq", split_axis=2, concat_axis=1, tiled=True))
    spectrum_grad, partials = mix_backward(
        flat_modes, hidden_pre, hidden, incoming, weights_in, weights_out
    )
    adjoint_part = jnp.einsum(
        "shkcd,wkc->shwd",
        lax.all_to_all(back_rows(spectrum_grad), "seq", split_axis=1, concat_axis=2, tiled=True),
        column_forward,
        preferred_element_type=jnp.float32,
    )
    mixed_out = (tokens.astype(jnp.float32) + mixed_grid).astype(jnp.bfloat16)
    tokens_grad = (cotangent.astype(jnp.float32) + adjoint_part).astype(jnp.bfloat16)
    totals = lax.psum((partials[0], partials[1], partials[2], partials[3]), ("seq", "rep"))
    divisor = float(samples * lax.axis_size("rep"))
    return (
        mixed_out,
        tokens_grad,
        totals[0] / divisor,
        totals[1] / divisor,
        totals[2] / divisor,
        totals[3] / divisor,
    )


GROUP = math.lcm(BLOCK, 128)
PER_GROUP = GROUP // BLOCK
COPY_A, COPY_B, COPY_C, COPY_E, COPY_F, COPY_G, COPY_H, COPY_D = range(8)
MESH_ID = pl.DeviceIdType.MESH
VMEM_LIMIT = 52 << 20


def host_tables(length, modes):
    residue = np.arange(length)[:, None] * np.arange(modes)[None, :] % length
    angles = residue.astype(np.float32) * np.float32(2.0 * math.pi / length)
    factor = np.float32(1.0 / math.sqrt(length))
    rounded = [(f(angles) * factor).astype(ml_dtypes.bfloat16) for f in (np.cos, np.sin)]
    return [table.astype(np.float32) for table in rounded]


def kernel_tables(width, length, n, samples, rows):
    local = MODES // n
    cosine, sine = host_tables(width, MODES)
    forward = np.stack([cosine.T, -sine.T], axis=1)
    doubled = forward * np.where(np.arange(MODES) == 0, 1.0, 2.0)[:, None, None]

    def spread(table):
        table = table.reshape(n, local, 2, width)
        whole = np.zeros((n, samples, local, 2, width, samples), np.float32)
        for s in range(samples):
            whole[:, s, :, :, :, s] = table
        return whole.reshape(n * samples * local * 2, width * samples)

    cosine, sine = host_tables(length, length)
    upper = np.stack([cosine, sine], axis=2)
    lower = np.stack([-sine, cosine], axis=2)
    turn = np.stack([upper, lower], axis=0)
    both = samples * local
    mixing = np.zeros((2, both, length, length, both, 2), np.float32)
    for x in range(both):
        mixing[:, x, :, :, x, :] = turn
    mixing = mixing.reshape(2 * both * length, length * both * 2)

    flat = [
        spread(forward),
        spread(doubled),
        spread(doubled).T,
        spread(forward).T,
        mixing,
    ]
    return [np.ascontiguousarray(t).astype(ml_dtypes.bfloat16) for t in flat]


def dot(a, b, contract=(1, 0)):
    return lax.dot_general(
        a, b, (((contract[0],), (contract[1],)), ((), ())), preferred_element_type=jnp.float32
    )


def mixer(
    n,
    inner,
    divisor,
    tok_far,
    cot_far,
    col_tok_far,
    col_cot_far,
    inv_mix_far,
    inv_grad_far,
    turn_far,
    in_weight_far,
    in_bias_far,
    out_weight_far,
    out_bias_far,
    mixed,
    grad,
    in_weight_grad,
    in_bias_grad,
    out_weight_grad,
    out_bias_grad,
    tok,
    cot,
    col_tok,
    col_cot,
    inv_mix,
    inv_grad,
    turn,
    in_weight,
    in_bias,
    out_weight,
    out_bias,
    send_a,
    send_b,
    send_c,
    send_d,
    send_e,
    send_f,
    recv_a,
    recv_b,
    recv_c,
    recv_d,
    recv_e,
    recv_f,
    turn_back,
    wide,
    spec,
    hid,
    slope,
    inc,
    pre,
    mixed_modes,
    grads,
    halves,
    half_in,
    part,
    gathered,
    other,
    both,
    send_sem,
    recv_sem,
    pair_send,
    pair_recv,
    load_sem,
):
    me = lax.axis_index("seq")
    core = lax.axis_index("rep")
    partner = 1 - core
    rows, width, samples, channels = tok.shape
    groups = channels // GROUP
    outer = n // inner
    across, within = me // inner, lax.rem(me, inner)
    chunk = send_a.shape[1]
    row_chunk = chunk // rows
    bf16 = jnp.bfloat16

    barrier = pltpu.get_barrier_semaphore()

    def greet(j, carry):
        peer = lax.rem(me + j, n)
        pl.semaphore_signal(barrier, inc=1, device_id={"seq": peer}, device_id_type=MESH_ID)
        return carry

    lax.fori_loop(1, n, greet, 0)
    pl.semaphore_signal(barrier, inc=1, device_id={"rep": partner}, device_id_type=MESH_ID)

    moves = [(col_tok_far, col_tok)]
    moves += [(tok_far.at[h], tok.at[h]) for h in range(rows)]
    moves += [(col_cot_far, col_cot)]
    moves += [(cot_far.at[h], cot.at[h]) for h in range(rows)]
    moves += [
        (in_weight_far, in_weight),
        (out_weight_far, out_weight),
        (turn_far, turn),
        (in_bias_far, in_bias),
        (out_bias_far, out_bias),
        (inv_mix_far, inv_mix),
        (inv_grad_far, inv_grad),
    ]
    loads = [
        pltpu.make_async_copy(far, near, load_sem.at[i]) for i, (far, near) in enumerate(moves)
    ]
    for load in loads:
        load.start()

    def copy_to(phase, peer, mine, source, target):
        return pltpu.make_async_remote_copy(
            src_ref=source,
            dst_ref=target,
            send_sem=send_sem.at[phase, peer],
            recv_sem=recv_sem.at[phase, mine],
            device_id={"seq": peer},
            device_id_type=MESH_ID,
        )

    def loop(count, act):
        def step(j, carry):
            act(j)
            return carry

        lax.fori_loop(1, count, step, 0)

    def peer_at(j):
        peer = jnp.int32(0)
        bit = 1
        while bit < n:
            peer = peer + bit * lax.rem(me // bit + j // bit, 2)
            bit *= 2
        return peer

    def plane_at(j):
        return lax.rem(within + j, inner)

    def line_at(j):
        return lax.rem(across + j, outer)

    def everyone(phase, source, target, at=None):
        cut = (lambda ref, i: ref.at[i]) if at is None else (lambda ref, i: ref.at[i, at])

        def out(j):
            peer = peer_at(j)
            return copy_to(phase, peer, me, cut(source, peer), cut(target, me))

        def back(j):
            peer = peer_at(j)
            return copy_to(phase, peer, peer, cut(source, peer), cut(target, peer))

        return (
            lambda: loop(n, lambda j: out(j).start()),
            lambda: loop(n, lambda j: back(j).wait_recv()),
            lambda: loop(n, lambda j: out(j).wait_send()),
        )

    def plane(phase, source, target):
        def out(j):
            v = plane_at(j)
            peer = across * inner + v
            return copy_to(phase, peer, me, source(v), target(within))

        def back(j):
            v = plane_at(j)
            peer = across * inner + v
            return copy_to(phase, peer, peer, source(v), target(v))

        return (
            lambda: loop(inner, lambda j: out(j).start()),
            lambda: loop(inner, lambda j: back(j).wait_recv()),
            lambda: loop(inner, lambda j: out(j).wait_send()),
        )

    def line(phase, source, target):
        def out(j):
            z = line_at(j)
            peer = z * inner + within
            return copy_to(phase, peer, me, source(z), target(across))

        def back(j):
            z = line_at(j)
            peer = z * inner + within
            return copy_to(phase, peer, peer, source(z), target(z))

        return (
            lambda: loop(outer, lambda j: out(j).start()),
            lambda: loop(outer, lambda j: back(j).wait_recv()),
            lambda: loop(outer, lambda j: out(j).wait_send()),
        )

    move_a = everyone(COPY_A, send_a, recv_a)
    move_b = everyone(COPY_B, send_b, recv_b)
    move_c = everyone(COPY_C, send_c, recv_c)
    pieces = [
        everyone(COPY_D + h, send_d, recv_d, pl.ds(h * row_chunk, row_chunk))
        for h in range(rows)
    ]
    move_e = plane(COPY_E, lambda v: send_e.at[v], lambda v: recv_e.at[v])
    move_f = line(COPY_F, lambda z: send_f.at[z], lambda z: recv_f.at[z])
    move_g = line(COPY_G, lambda z: part, lambda z: gathered.at[within, z])
    move_h = plane(COPY_H, lambda v: gathered.at[within], lambda v: gathered.at[v])

    def columns(tokens, table, send, arrived):
        arrived[0].wait()
        for h in range(rows):
            arrived[1 + h].wait()
            product = dot(table[...], tokens[h].reshape(width * samples, channels))
            send[:, h * row_chunk : (h + 1) * row_chunk, :] = product.astype(bf16).reshape(
                n, row_chunk, channels
            )

    columns(tok, col_tok, send_a, loads[: rows + 1])
    pl.semaphore_wait(barrier, n)
    move_a[0]()
    columns(cot, col_cot, send_b, loads[rows + 1 : 2 * rows + 2])
    move_b[0]()
    for load in loads[2 * rows + 2 :]:
        load.wait()
    recv_a[me] = send_a[me]
    recv_b[me] = send_b[me]

    turn_back[...] = turn[...].T
    row_at = lax.broadcasted_iota(jnp.int32, (BLOCK, GROUP), 0)
    lane_at = lax.broadcasted_iota(jnp.int32, (BLOCK, GROUP), 1)
    for at, weight in enumerate((in_weight, out_weight)):
        for i in range(PER_GROUP):
            place = (lane_at == row_at + i * BLOCK).astype(bf16)
            for c in range(2):
                for g in range(groups):
                    wide[2 * at + c, g, i * BLOCK : (i + 1) * BLOCK, :] = dot(
                        weight[c, g * PER_GROUP + i], place
                    ).astype(bf16)

    half = turn.shape[0] // 2
    scale = math.sqrt(2.0 / math.pi)

    def lanes(g):
        return pl.ds(pl.multiple_of(g * GROUP, GROUP), GROUP)

    def per_group(act):
        def step(g, carry):
            act(g, lanes(g))
            return carry

        lax.fori_loop(0, groups, step, 0)

    def along_rows(recv, at, keep, g):
        keep[g] = dot(turn[...], recv[:, :, at].reshape(turn.shape[1], GROUP)).astype(bf16)

    def back_rows(send, at):
        send[:, :, at] = (
            dot(turn_back[...], mixed_modes[...]).astype(bf16).reshape(n, chunk, GROUP)
        )

    def forward_group(g, at):
        along_rows(recv_a, at, spec, g)
        re, im = spec[g, :half], spec[g, half:]
        w_re, w_im = wide[0, g], wide[1, g]
        for c in range(2):
            if c == 0:
                value = dot(re, w_re) - dot(im, w_im)
            else:
                value = dot(re, w_im) + dot(im, w_re)
            value = value + in_bias[c : c + 1, at]
            square = value * value
            tanh = jnp.tanh(scale * value * (1.0 + 0.044715 * square))
            hid[g, c * half : (c + 1) * half] = (0.5 * value * (1.0 + tanh)).astype(bf16)
            slope[g, c * half : (c + 1) * half] = 0.5 * (1.0 + tanh) + 0.5 * value * (
                1.0 - tanh * tanh
            ) * (scale * (1.0 + (3.0 * 0.044715) * square))
        re, im = hid[g, :half], hid[g, half:]
        w_re, w_im = wide[2, g], wide[3, g]
        mixed_modes[:half] = (
            dot(re, w_re) - dot(im, w_im) + out_bias[0:1, at]
        ).astype(bf16)
        mixed_modes[half:] = (
            dot(re, w_im) + dot(im, w_re) + out_bias[1:2, at]
        ).astype(bf16)
        back_rows(send_c, at)

    move_a[1]()
    per_group(forward_group)
    move_c[0]()
    recv_c[me] = send_c[me]

    def backward_group(g, at):
        along_rows(recv_b, at, inc, g)
        re, im = inc[g, :half], inc[g, half:]
        w_re, w_im = wide[2, g], wide[3, g]
        pre[g, :half] = (
            (dot(re, w_re, (1, 1)) + dot(im, w_im, (1, 1))) * slope[g, :half]
        ).astype(bf16)
        pre[g, half:] = (
            (dot(im, w_re, (1, 1)) - dot(re, w_im, (1, 1))) * slope[g, half:]
        ).astype(bf16)
        re, im = pre[g, :half], pre[g, half:]
        w_re, w_im = wide[0, g], wide[1, g]
        mixed_modes[:half] = (dot(re, w_re, (1, 1)) + dot(im, w_im, (1, 1))).astype(bf16)
        mixed_modes[half:] = (dot(im, w_re, (1, 1)) - dot(re, w_im, (1, 1))).astype(bf16)
        back_rows(send_d, at)

    move_b[1]()
    per_group(backward_group)
    pieces[0][0]()
    recv_d[me] = send_d[me]

    def fold(product):
        total = jnp.zeros((BLOCK, GROUP), jnp.float32)
        for i in range(PER_GROUP):
            inside = (lane_at >= i * BLOCK) & (lane_at < (i + 1) * BLOCK)
            total = jnp.where(inside, product[i * BLOCK : (i + 1) * BLOCK], total)
        return total.astype(bf16)

    bias_at = lax.broadcasted_iota(jnp.int32, (16, GROUP), 0)

    def grads_group(g, at):
        bias = jnp.zeros((16, GROUP), jnp.float32)
        for k, (left, right) in enumerate(((spec, pre), (hid, inc))):
            a_re, a_im = left[g, :half], left[g, half:]
            b_re, b_im = right[g, :half], right[g, half:]
            first = 2 * k * BLOCK
            grads[first : first + BLOCK, at] = fold(
                dot(a_re, b_re, (0, 0)) + dot(a_im, b_im, (0, 0))
            )
            grads[first + BLOCK : first + 2 * BLOCK, at] = fold(
                dot(a_re, b_im, (0, 0)) - dot(a_im, b_re, (0, 0))
            )
            for c, value in enumerate((b_re, b_im)):
                total = jnp.sum(value.astype(jnp.float32), axis=0, keepdims=True)
                bias = jnp.where(bias_at == 2 * k + c, total, bias)
        grads[4 * BLOCK : 4 * BLOCK + 16, at] = bias.astype(bf16)

    per_group(grads_group)
    per = 4 * BLOCK // (2 * n)
    to_row = lax.broadcasted_iota(jnp.int32, (2 * n * 16, 4 * BLOCK + 16), 0)
    from_row = lax.broadcasted_iota(jnp.int32, (2 * n * 16, 4 * BLOCK + 16), 1)
    slot = to_row % 16
    wanted = jnp.where(slot < per, to_row // 16 * per + slot, 4 * BLOCK + slot - per)
    picks = (wanted == from_row).astype(bf16)
    halves[...] = dot(picks, grads[...]).astype(bf16).reshape(halves.shape)

    def swap(slot, source, target):
        return pltpu.make_async_remote_copy(
            src_ref=source,
            dst_ref=target,
            send_sem=pair_send.at[slot],
            recv_sem=pair_recv.at[slot],
            device_id={"rep": partner},
            device_id_type=MESH_ID,
        )

    first_swap = swap(0, halves.at[partner], half_in)
    first_swap.start()

    def inverse_row(h, tokens, table, recv, out):
        section = recv[:, h * row_chunk : (h + 1) * row_chunk, :]
        product = dot(table[...], section.reshape(n * row_chunk, channels))
        kept = tokens[h].reshape(width * samples, channels).astype(jnp.float32)
        out[h] = (kept + product).astype(bf16).reshape(width, samples, channels)

    def inverse(tokens, table, recv, out):
        for h in range(rows):
            inverse_row(h, tokens, table, recv, out)

    first_swap.wait()
    send_e[...] = (
        (halves[core].astype(jnp.float32) + half_in[...].astype(jnp.float32))
        .astype(bf16)
        .reshape(send_e.shape)
    )
    move_e[0]()
    recv_e[within] = send_e[within]
    move_c[1]()
    inverse(tok, inv_mix, recv_c, mixed)

    move_e[1]()
    send_f[...] = jnp.sum(recv_e[...].astype(jnp.float32), axis=0).astype(bf16)
    move_f[0]()
    recv_f[across] = send_f[across]
    middle = max(2, rows - 1)
    for piece in pieces[1:middle]:
        piece[0]()
    move_f[1]()
    total = jnp.sum(recv_f[...].astype(jnp.float32), axis=0) * (1.0 / divisor)
    in_bias_grad[...] = total[per : per + 2]
    out_bias_grad[...] = total[per + 2 : per + 4]
    part[...] = total.astype(bf16)
    move_g[0]()
    gathered[within, across] = part[...]
    for piece in pieces[middle:]:
        piece[0]()
    pieces[0][1]()
    inverse_row(0, cot, inv_grad, recv_d, grad)
    move_g[1]()
    move_h[0]()
    for h in range(1, rows - 1):
        pieces[h][1]()
        inverse_row(h, cot, inv_grad, recv_d, grad)
    move_h[1]()
    last_swap = swap(1, gathered, other)
    last_swap.start()
    both[core] = gathered[...].reshape(n * 16, channels)
    for move in (move_a, move_b, move_c, move_e, move_f, move_g, move_h):
        move[2]()
    for h in range(max(1, rows - 1), rows):
        pieces[h][1]()
        inverse_row(h, cot, inv_grad, recv_d, grad)
    last_swap.wait()
    both[partner] = other[...].reshape(n * 16, channels)
    to_row = lax.broadcasted_iota(jnp.int32, (2 * BLOCK, n * 16), 0)
    from_row = lax.broadcasted_iota(jnp.int32, (2 * BLOCK, n * 16), 1)
    order = (to_row // per * 16 + to_row % per == from_row).astype(bf16)
    for k, out in enumerate((in_weight_grad, out_weight_grad)):
        for g in range(groups):
            ordered = dot(order, both[k, :, g * GROUP : (g + 1) * GROUP]).astype(bf16)
            for i in range(PER_GROUP):
                place = (lane_at == row_at + i * BLOCK).astype(bf16)
                block = dot(ordered, place, (1, 1))
                for c in range(2):
                    out[c, g * PER_GROUP + i] = block[c * BLOCK : (c + 1) * BLOCK]

    for move in pieces:
        move[2]()


def settle(*refs):
    count = len(refs) // 2
    near, far, sems = refs[:count], refs[count:-1], refs[-1]
    copies = [
        pltpu.make_async_copy(a, b, sems.at[i]) for i, (a, b) in enumerate(zip(near, far))
    ]
    for copy in copies:
        copy.start()
    for copy in copies:
        copy.wait()


def fits(n, reps, samples, rows, channels):
    per_row = samples * (MODES // n) * 2
    return (
        reps == 2
        and MODES % n == 0
        and per_row % 16 == 0
        and channels % GROUP == 0
        and channels == BLOCKS * BLOCK
        and (4 * BLOCK) % (2 * n) == 0
        and n > 1
        and n & (n - 1) == 0
        and rows > 1
        and 4 * BLOCK // (2 * n) + 4 <= 16
        and (samples * MODES // n * rows * n) % 16 == 0
    )


def shards(tokens, cotangent, in_weight, in_bias, out_weight, out_bias):
    samples, rows, width, channels = tokens.shape
    n, reps = lax.axis_size("seq"), lax.axis_size("rep")
    if not fits(n, reps, samples, rows, channels):
        return shards_plain(tokens, cotangent, in_weight, in_bias, out_weight, out_bias)
    length = rows * n
    inner = 2 ** ((n.bit_length() - 1) // 2)
    outer = n // inner
    chunk = rows * samples * (MODES // n) * 2
    whole = n * chunk
    groups = channels // GROUP
    tables = [jnp.asarray(t) for t in kernel_tables(width, length, n, samples, rows)]
    bf16, f32 = jnp.bfloat16, jnp.float32
    block = pltpu.VMEM((n, chunk, channels), bf16)
    small = pltpu.VMEM((n, 16, channels), bf16)
    ringed = pltpu.VMEM((inner, outer, 16, channels), bf16)
    lined = pltpu.VMEM((outer, 16, channels), bf16)
    planes = (tokens.transpose(1, 2, 0, 3), cotangent.transpose(1, 2, 0, 3))
    kept = pltpu.VMEM((groups, whole, GROUP), bf16)
    vmem = pl.BlockSpec(memory_space=pltpu.VMEM)
    far = pl.BlockSpec(memory_space=pltpu.HBM)
    inputs = (*planes, *tables, in_weight, in_bias, out_weight, out_bias)
    shapes = (
        (planes[0].shape, bf16),
        (planes[1].shape, bf16),
        (in_weight.shape, f32),
        (in_bias.shape, f32),
        (out_weight.shape, f32),
        (out_bias.shape, f32),
    )
    near = pl.pallas_call(
        functools.partial(mixer, n, inner, float(samples * reps)),
        out_shape=tuple(pltpu.VMEM(*shape) for shape in shapes),
        in_specs=[far] * 11,
        out_specs=(vmem,) * 6,
        scratch_shapes=[pltpu.VMEM(v.shape, v.dtype) for v in inputs]
        + [block] * 4
        + [ringed, lined]
        + [block] * 4
        + [ringed, lined]
        + [
            pltpu.VMEM((whole, whole), bf16),
            pltpu.VMEM((4, groups, GROUP, GROUP), bf16),
            kept,
            kept,
            pltpu.VMEM((groups, whole, GROUP), f32),
            kept,
            kept,
            pltpu.VMEM((whole, GROUP), bf16),
            pltpu.VMEM((4 * BLOCK + 16, channels), bf16),
            pltpu.VMEM((2, n, 16, channels), bf16),
            small,
            pltpu.VMEM((16, channels), bf16),
            ringed,
            ringed,
            pltpu.VMEM((2, n * 16, channels), bf16),
            pltpu.SemaphoreType.DMA((COPY_D + rows, n)),
            pltpu.SemaphoreType.DMA((COPY_D + rows, n)),
            pltpu.SemaphoreType.DMA((2,)),
            pltpu.SemaphoreType.DMA((2,)),
            pltpu.SemaphoreType.DMA((2 * rows + 9,)),
        ],
        compiler_params=pltpu.CompilerParams(
            collective_id=0, has_side_effects=True, vmem_limit_bytes=VMEM_LIMIT
        ),
        name="mixer",
    )(*inputs)
    mixed, grad, *parameter_grads = pl.pallas_call(
        settle,
        out_shape=tuple(jax.ShapeDtypeStruct(*shape) for shape in shapes),
        in_specs=[pl.BlockSpec(memory_space=pl.ANY)] * 6,
        out_specs=(far,) * 6,
        scratch_shapes=[pltpu.SemaphoreType.DMA((6,))],
        compiler_params=pltpu.CompilerParams(vmem_limit_bytes=1 << 20),
        name="settle",
    )(*(pltpu.with_memory_space_constraint(part, pltpu.VMEM) for part in near))
    return (
        mixed.transpose(2, 0, 1, 3),
        grad.transpose(2, 0, 1, 3),
        *parameter_grads,
    )


def solution(mesh):
    in_specs = (P("rep", "seq", None, None), P("rep", "seq", None, None), P(), P(), P(), P())
    out_specs = (P("rep", "seq", None, None), P("rep", "seq", None, None), P(), P(), P(), P())
    return jax.shard_map(shards, mesh=mesh, in_specs=in_specs, out_specs=out_specs, check_vma=False)
```

```python
import functools
import math

import jax
import jax.numpy as jnp
import ml_dtypes
import numpy as np
from jax import lax
from jax.experimental import pallas as pl
from jax.experimental.pallas import tpu as pltpu
from jax.sharding import PartitionSpec as P

BLOCKS = 8
BLOCK = 96
MODES = 64


def grid_tables(length, modes):
    position = jnp.arange(length, dtype=jnp.int32)
    frequency = jnp.arange(modes, dtype=jnp.int32)
    residue = position[:, None] * frequency[None, :] % length
    angles = residue.astype(jnp.float32) * (2.0 * math.pi / length)
    factor = 1.0 / math.sqrt(length)
    cosine_table = (jnp.cos(angles) * factor).astype(jnp.bfloat16)
    sine_table = (jnp.sin(angles) * factor).astype(jnp.bfloat16)
    return (cosine_table, sine_table)


def column_tables(grid_width, modes):
    cosine_table, sine_table = grid_tables(grid_width, modes)
    forward = jnp.stack([cosine_table, -sine_table], axis=2)
    doubling = jnp.where(jnp.arange(modes) == 0, 1.0, 2.0).astype(jnp.bfloat16)[:, None]
    inverse = jnp.stack([cosine_table.T * doubling, -(sine_table.T * doubling)], axis=1)
    return (forward, inverse)


def row_table(length):
    cosine_table, sine_table = grid_tables(length, length)
    upper_rows = jnp.stack([cosine_table, sine_table], axis=2)
    lower_rows = jnp.stack([-sine_table, cosine_table], axis=2)
    return jnp.stack([upper_rows, lower_rows], axis=1)


def block_weights(weight):
    real_part, imag_part = (weight[0], weight[1])
    upper_half = jnp.stack([real_part, imag_part], axis=2)
    lower_half = jnp.stack([-imag_part, real_part], axis=2)
    return jnp.stack([upper_half, lower_half], axis=1)


def fold_blocks(blockwise):
    real_part = blockwise[:, 0, :, 0, :] + blockwise[:, 1, :, 1, :]
    imag_part = blockwise[:, 0, :, 1, :] - blockwise[:, 1, :, 0, :]
    return jnp.stack([real_part, imag_part])


def mix_forward(spectrum, weights_in, weights_out, bias_in, bias_out):
    mode_count = spectrum.shape[0] * spectrum.shape[1] * spectrum.shape[2]
    flat_modes = spectrum.reshape(mode_count, 2, BLOCKS, BLOCK)
    hidden_pre = (
        jnp.einsum("mcbi,bciej->mebj", flat_modes, weights_in, preferred_element_type=jnp.float32)
        + bias_in
    )
    hidden = jax.nn.gelu(hidden_pre).astype(jnp.bfloat16)
    spectrum_out = (
        jnp.einsum("mcbi,bciej->mebj", hidden, weights_out, preferred_element_type=jnp.float32)
        + bias_out
    )
    return (
        flat_modes,
        hidden_pre,
        hidden,
        spectrum_out.astype(jnp.bfloat16).reshape(spectrum.shape),
    )


def mix_backward(flat_modes, hidden_pre, hidden, incoming, weights_in, weights_out):
    incoming_flat = incoming.reshape(flat_modes.shape)
    out_bias_part = jnp.sum(incoming_flat.astype(jnp.float32), axis=0).reshape(2, -1)
    out_weight_part = fold_blocks(
        jnp.einsum("mcbi,mebj->bciej", hidden, incoming_flat, preferred_element_type=jnp.float32)
    )
    hidden_grad = jnp.einsum(
        "mebj,bciej->mcbi", incoming_flat, weights_out, preferred_element_type=jnp.float32
    )
    pre_grad = jax.vjp(jax.nn.gelu, hidden_pre)[1](hidden_grad)[0].astype(jnp.bfloat16)
    in_bias_part = jnp.sum(pre_grad.astype(jnp.float32), axis=0).reshape(2, -1)
    in_weight_part = fold_blocks(
        jnp.einsum("mcbi,mebj->bciej", flat_modes, pre_grad, preferred_element_type=jnp.float32)
    )
    spectrum_grad = jnp.einsum(
        "mebj,bciej->mcbi", pre_grad, weights_in, preferred_element_type=jnp.float32
    )
    spectrum_grad = spectrum_grad.astype(jnp.bfloat16).reshape(incoming.shape)
    return (spectrum_grad, (in_weight_part, in_bias_part, out_weight_part, out_bias_part))


def shards_plain(tokens, cotangent, in_weight, in_bias, out_weight, out_bias):
    samples, row_count, grid_width, channels = tokens.shape
    length = row_count * lax.axis_size("seq")
    column_forward, column_inverse = column_tables(grid_width, MODES)
    row_matrix = row_table(length)
    weights_in = block_weights(in_weight)
    weights_out = block_weights(out_weight)
    bias_in = in_bias.reshape(2, BLOCKS, BLOCK)
    bias_out = out_bias.reshape(2, BLOCKS, BLOCK)

    def along_rows(section):
        return jnp.einsum(
            "qehc,shkcd->sqked", row_matrix, section, preferred_element_type=jnp.float32
        ).astype(jnp.bfloat16)

    def back_rows(section):
        return jnp.einsum(
            "qehc,sqked->shkcd", row_matrix, section, preferred_element_type=jnp.float32
        ).astype(jnp.bfloat16)

    spec_rows = jnp.einsum(
        "shwd,wkc->shkcd", tokens, column_forward, preferred_element_type=jnp.float32
    ).astype(jnp.bfloat16)
    spectrum = along_rows(lax.all_to_all(spec_rows, "seq", split_axis=2, concat_axis=1, tiled=True))
    flat_modes, hidden_pre, hidden, spectrum_out = mix_forward(
        spectrum, weights_in, weights_out, bias_in, bias_out
    )
    mixed_grid = jnp.einsum(
        "shkcd,kcw->shwd",
        lax.all_to_all(back_rows(spectrum_out), "seq", split_axis=1, concat_axis=2, tiled=True),
        column_inverse,
        preferred_element_type=jnp.float32,
    )
    cot_rows = jnp.einsum(
        "shwd,kcw->shkcd", cotangent, column_inverse, preferred_element_type=jnp.float32
    ).astype(jnp.bfloat16)
    incoming = along_rows(lax.all_to_all(cot_rows, "seq", split_axis=2, concat_axis=1, tiled=True))
    spectrum_grad, partials = mix_backward(
        flat_modes, hidden_pre, hidden, incoming, weights_in, weights_out
    )
    adjoint_part = jnp.einsum(
        "shkcd,wkc->shwd",
        lax.all_to_all(back_rows(spectrum_grad), "seq", split_axis=1, concat_axis=2, tiled=True),
        column_forward,
        preferred_element_type=jnp.float32,
    )
    mixed_out = (tokens.astype(jnp.float32) + mixed_grid).astype(jnp.bfloat16)
    tokens_grad = (cotangent.astype(jnp.float32) + adjoint_part).astype(jnp.bfloat16)
    totals = lax.psum((partials[0], partials[1], partials[2], partials[3]), ("seq", "rep"))
    divisor = float(samples * lax.axis_size("rep"))
    return (
        mixed_out,
        tokens_grad,
        totals[0] / divisor,
        totals[1] / divisor,
        totals[2] / divisor,
        totals[3] / divisor,
    )


GROUP = math.lcm(BLOCK, 128)
PER_GROUP = GROUP // BLOCK
MESH_ID = pl.DeviceIdType.MESH
VMEM_LIMIT = 52 << 20


def host_tables(length, modes):
    residue = np.arange(length)[:, None] * np.arange(modes)[None, :] % length
    angles = residue.astype(np.float32) * np.float32(2.0 * math.pi / length)
    factor = np.float32(1.0 / math.sqrt(length))
    rounded = [(f(angles) * factor).astype(ml_dtypes.bfloat16) for f in (np.cos, np.sin)]
    return [table.astype(np.float32) for table in rounded]


def kernel_tables(width, length, n, samples, rows):
    local = MODES // n
    cosine, sine = host_tables(width, MODES)
    forward = np.stack([cosine.T, -sine.T], axis=1)
    doubled = forward * np.where(np.arange(MODES) == 0, 1.0, 2.0)[:, None, None]

    def spread(table):
        table = table.reshape(n, local, 2, width)
        whole = np.zeros((n, samples, local, 2, width, samples), np.float32)
        for s in range(samples):
            whole[:, s, :, :, :, s] = table
        return whole.reshape(n * samples * local * 2, width * samples)

    cosine, sine = host_tables(length, length)
    upper = np.stack([cosine, sine], axis=2)
    lower = np.stack([-sine, cosine], axis=2)
    turn = np.stack([upper, lower], axis=0)
    both = samples * local
    mixing = np.zeros((2, both, length, length, both, 2), np.float32)
    for x in range(both):
        mixing[:, x, :, :, x, :] = turn
    mixing = mixing.reshape(2 * both * length, length * both * 2)

    flat = [
        spread(forward),
        spread(doubled),
        spread(doubled).T,
        spread(forward).T,
        mixing,
    ]
    return [np.ascontiguousarray(t).astype(ml_dtypes.bfloat16) for t in flat]


def dot(a, b, contract=(1, 0)):
    return lax.dot_general(
        a, b, (((contract[0],), (contract[1],)), ((), ())), preferred_element_type=jnp.float32
    )


def mixer(
    n,
    inner,
    divisor,
    tok_far,
    cot_far,
    col_tok_far,
    col_cot_far,
    inv_mix_far,
    inv_grad_far,
    turn_far,
    in_weight_far,
    in_bias_far,
    out_weight_far,
    out_bias_far,
    mixed,
    grad,
    in_weight_grad,
    in_bias_grad,
    out_weight_grad,
    out_bias_grad,
    tok,
    cot,
    col_tok,
    col_cot,
    inv_mix,
    inv_grad,
    turn,
    in_weight,
    in_bias,
    out_weight,
    out_bias,
    send_a,
    send_b,
    send_c,
    send_d,
    recv_a,
    recv_b,
    recv_c,
    recv_d,
    send_e,
    send_f,
    recv_e,
    recv_f,
    turn_back,
    wide,
    spec,
    hid,
    slope,
    inc,
    pre,
    mixed_modes,
    grads,
    halves,
    half_in,
    part,
    gathered,
    other,
    both,
    send_sem,
    recv_sem,
    pair_send,
    pair_recv,
    load_sem,
):
    me = lax.axis_index("seq")
    core = lax.axis_index("rep")
    partner = 1 - core
    rows, width, samples, channels = tok.shape
    groups = channels // GROUP
    outer = n // inner
    across, within = me // inner, lax.rem(me, inner)
    chunk = send_a.shape[2]
    row_chunk = chunk // rows
    bf16 = jnp.bfloat16

    barrier = pltpu.get_barrier_semaphore()

    def greet(j, carry):
        peer = lax.rem(me + j, n)
        pl.semaphore_signal(barrier, inc=1, device_id={"seq": peer}, device_id_type=MESH_ID)
        return carry

    lax.fori_loop(1, n, greet, 0)
    pl.semaphore_signal(barrier, inc=1, device_id={"rep": partner}, device_id_type=MESH_ID)

    moves = [(col_tok_far, col_tok)]
    moves += [(tok_far.at[h], tok.at[h]) for h in range(rows)]
    moves += [(col_cot_far, col_cot)]
    moves += [(cot_far.at[h], cot.at[h]) for h in range(rows)]
    moves += [
        (in_weight_far, in_weight),
        (out_weight_far, out_weight),
        (turn_far, turn),
        (in_bias_far, in_bias),
        (out_bias_far, out_bias),
        (inv_mix_far, inv_mix),
        (inv_grad_far, inv_grad),
    ]
    loads = [
        pltpu.make_async_copy(far, near, load_sem.at[i]) for i, (far, near) in enumerate(moves)
    ]
    for load in loads:
        load.start()

    def copy_to(slot, peer, source, target):
        return pltpu.make_async_remote_copy(
            src_ref=source,
            dst_ref=target,
            send_sem=send_sem.at[slot],
            recv_sem=recv_sem.at[slot],
            device_id={"seq": peer},
            device_id_type=MESH_ID,
        )

    def loop(count, act):
        def step(j, carry):
            act(j)
            return carry

        lax.fori_loop(1, count, step, 0)

    def peer_at(j):
        peer = jnp.int32(0)
        bit = 1
        while bit < n:
            peer = peer + bit * lax.rem(me // bit + j // bit, 2)
            bit *= 2
        return peer

    class Move:
        def __init__(self, slot, count, to, source, target, span):
            self.slot, self.count, self.to = slot, count, to
            self.source, self.target, self.span = source, target, span

        def start(self):
            def out(j):
                at, peer = self.to(j)
                copy_to(self.slot, peer, self.source(at), self.target).start()

            loop(self.count, out)

        def all(self):
            return copy_to(self.slot, me, self.span, self.span)

        def arrived(self):
            self.all().wait_recv()

        def left(self):
            self.all().wait_send()

    def to_peer(j):
        peer = peer_at(j)
        return peer, peer

    def to_plane(j):
        v = lax.rem(within + j, inner)
        return v, across * inner + v

    def to_line(j):
        z = lax.rem(across + j, outer)
        return z, z * inner + within

    def everyone(slot, source, target, g, at=None):
        cut = pl.ds(0, chunk) if at is None else at
        return Move(
            slot,
            n,
            to_peer,
            lambda peer: source.at[g, peer, cut],
            target.at[g, me, cut],
            target.at[g, pl.ds(0, n - 1), cut],
        )

    def move_a(g):
        return everyone(g, send_a, recv_a, g)

    def move_b(g):
        return everyone(groups + g, send_b, recv_b, g)

    def move_c(g):
        return everyone(2 * groups + g, send_c, recv_c, g)

    def move_d(g, h):
        return everyone(
            3 * groups + g * rows + h, send_d, recv_d, g, pl.ds(h * row_chunk, row_chunk)
        )

    tail = 3 * groups + rows * groups
    move_e = Move(
        tail,
        inner,
        to_plane,
        lambda v: send_e.at[v],
        recv_e.at[within],
        recv_e.at[pl.ds(0, inner - 1)],
    )
    move_f = Move(
        tail + 1,
        outer,
        to_line,
        lambda z: send_f.at[z],
        recv_f.at[across],
        recv_f.at[pl.ds(0, outer - 1)],
    )
    move_g = Move(
        tail + 2,
        outer,
        to_line,
        lambda z: part,
        gathered.at[within, across],
        gathered.at[within, pl.ds(0, outer - 1)],
    )
    move_h = Move(
        tail + 3,
        inner,
        to_plane,
        lambda v: gathered.at[within],
        gathered.at[within],
        gathered.at[pl.ds(0, inner - 1)],
    )

    def lanes(g):
        return pl.ds(pl.multiple_of(g * GROUP, GROUP), GROUP)

    def fixed(g):
        return pl.ds(g * GROUP, GROUP)

    def columns(tokens, table, send, g, arrived):
        for h in range(rows):
            if arrived:
                arrived[h].wait()
            section = tokens[h, :, :, fixed(g)].reshape(width * samples, GROUP)
            send[g, :, h * row_chunk : (h + 1) * row_chunk, :] = (
                dot(table[...], section).astype(bf16).reshape(n, row_chunk, GROUP)
            )

    for g in range(groups):
        if g == 0:
            loads[0].wait()
        columns(tok, col_tok, send_a, g, loads[1 : rows + 1] if g == 0 else None)
        if g == 0:
            pl.semaphore_wait(barrier, n)
        move_a(g).start()
        if g == 0:
            loads[rows + 1].wait()
        columns(cot, col_cot, send_b, g, loads[rows + 2 : 2 * rows + 2] if g == 0 else None)
        move_b(g).start()
    for load in loads[2 * rows + 2 :]:
        load.wait()
    recv_a[:, me] = send_a[:, me]
    recv_b[:, me] = send_b[:, me]

    turn_back[...] = turn[...].T
    row_at = lax.broadcasted_iota(jnp.int32, (BLOCK, GROUP), 0)
    lane_at = lax.broadcasted_iota(jnp.int32, (BLOCK, GROUP), 1)
    for at, weight in enumerate((in_weight, out_weight)):
        for i in range(PER_GROUP):
            place = (lane_at == row_at + i * BLOCK).astype(bf16)
            for c in range(2):
                for g in range(groups):
                    wide[2 * at + c, g, i * BLOCK : (i + 1) * BLOCK, :] = dot(
                        weight[c, g * PER_GROUP + i], place
                    ).astype(bf16)

    half = turn.shape[0] // 2
    scale = math.sqrt(2.0 / math.pi)

    def per_group(act):
        def step(g, carry):
            act(g, lanes(g))
            return carry

        lax.fori_loop(0, groups, step, 0)

    def along_rows(recv, keep, g):
        keep[g] = dot(turn[...], recv[g].reshape(turn.shape[1], GROUP)).astype(bf16)

    def back_rows(send, g):
        send[g] = dot(turn_back[...], mixed_modes[...]).astype(bf16).reshape(n, chunk, GROUP)

    def forward_group(g, at):
        along_rows(recv_a, spec, g)
        re, im = spec[g, :half], spec[g, half:]
        w_re, w_im = wide[0, g], wide[1, g]
        for c in range(2):
            if c == 0:
                value = dot(re, w_re) - dot(im, w_im)
            else:
                value = dot(re, w_im) + dot(im, w_re)
            value = value + in_bias[c : c + 1, at]
            square = value * value
            tanh = jnp.tanh(scale * value * (1.0 + 0.044715 * square))
            hid[g, c * half : (c + 1) * half] = (0.5 * value * (1.0 + tanh)).astype(bf16)
            slope[g, c * half : (c + 1) * half] = 0.5 * (1.0 + tanh) + 0.5 * value * (
                1.0 - tanh * tanh
            ) * (scale * (1.0 + (3.0 * 0.044715) * square))
        re, im = hid[g, :half], hid[g, half:]
        w_re, w_im = wide[2, g], wide[3, g]
        mixed_modes[:half] = (
            dot(re, w_re) - dot(im, w_im) + out_bias[0:1, at]
        ).astype(bf16)
        mixed_modes[half:] = (
            dot(re, w_im) + dot(im, w_re) + out_bias[1:2, at]
        ).astype(bf16)
        back_rows(send_c, g)

    def backward_group(g):
        along_rows(recv_b, inc, g)
        re, im = inc[g, :half], inc[g, half:]
        w_re, w_im = wide[2, g], wide[3, g]
        pre[g, :half] = (
            (dot(re, w_re, (1, 1)) + dot(im, w_im, (1, 1))) * slope[g, :half]
        ).astype(bf16)
        pre[g, half:] = (
            (dot(im, w_re, (1, 1)) - dot(re, w_im, (1, 1))) * slope[g, half:]
        ).astype(bf16)
        re, im = pre[g, :half], pre[g, half:]
        w_re, w_im = wide[0, g], wide[1, g]
        mixed_modes[:half] = (dot(re, w_re, (1, 1)) + dot(im, w_im, (1, 1))).astype(bf16)
        mixed_modes[half:] = (dot(im, w_re, (1, 1)) - dot(re, w_im, (1, 1))).astype(bf16)
        back_rows(send_d, g)

    def fold(product):
        total = jnp.zeros((BLOCK, GROUP), jnp.float32)
        for i in range(PER_GROUP):
            inside = (lane_at >= i * BLOCK) & (lane_at < (i + 1) * BLOCK)
            total = jnp.where(inside, product[i * BLOCK : (i + 1) * BLOCK], total)
        return total.astype(bf16)

    bias_at = lax.broadcasted_iota(jnp.int32, (16, GROUP), 0)

    def grads_group(g, at):
        bias = jnp.zeros((16, GROUP), jnp.float32)
        for k, (left, right) in enumerate(((spec, pre), (hid, inc))):
            a_re, a_im = left[g, :half], left[g, half:]
            b_re, b_im = right[g, :half], right[g, half:]
            first = 2 * k * BLOCK
            grads[first : first + BLOCK, at] = fold(
                dot(a_re, b_re, (0, 0)) + dot(a_im, b_im, (0, 0))
            )
            grads[first + BLOCK : first + 2 * BLOCK, at] = fold(
                dot(a_re, b_im, (0, 0)) - dot(a_im, b_re, (0, 0))
            )
            for c, value in enumerate((b_re, b_im)):
                total = jnp.sum(value.astype(jnp.float32), axis=0, keepdims=True)
                bias = jnp.where(bias_at == 2 * k + c, total, bias)
        grads[4 * BLOCK : 4 * BLOCK + 16, at] = bias.astype(bf16)

    def mix_group(g, at):
        with jax.named_scope("wait_a"):
            move_a(g).arrived()
        with jax.named_scope("fwd"):
            forward_group(g, at)
        move_c(g).start()
        recv_c[g, me] = send_c[g, me]
        with jax.named_scope("wait_b"):
            move_b(g).arrived()
        with jax.named_scope("bwd"):
            backward_group(g)
        recv_d[g, me] = send_d[g, me]

        @pl.when(g < groups - 1)
        def _():
            for h in range(rows):
                move_d(g, h).start()

        with jax.named_scope("grads"):
            grads_group(g, at)

    per_group(mix_group)

    per = 4 * BLOCK // (2 * n)
    to_row = lax.broadcasted_iota(jnp.int32, (2 * n * 16, 4 * BLOCK + 16), 0)
    from_row = lax.broadcasted_iota(jnp.int32, (2 * n * 16, 4 * BLOCK + 16), 1)
    slot = to_row % 16
    wanted = jnp.where(slot < per, to_row // 16 * per + slot, 4 * BLOCK + slot - per)
    picks = (wanted == from_row).astype(bf16)
    halves[...] = dot(picks, grads[...]).astype(bf16).reshape(halves.shape)

    def swap(slot, source, target):
        return pltpu.make_async_remote_copy(
            src_ref=source,
            dst_ref=target,
            send_sem=pair_send.at[slot],
            recv_sem=pair_recv.at[slot],
            device_id={"rep": partner},
            device_id_type=MESH_ID,
        )

    first_swap = swap(0, halves.at[partner], half_in)
    first_swap.start()

    def inverse_row(h, g, tokens, table, recv, out):
        section = recv[g, :, h * row_chunk : (h + 1) * row_chunk, :]
        product = dot(table[...], section.reshape(n * row_chunk, GROUP))
        kept = tokens[h, :, :, fixed(g)].reshape(width * samples, GROUP).astype(jnp.float32)
        out[h, :, :, fixed(g)] = (kept + product).astype(bf16).reshape(width, samples, GROUP)

    with jax.named_scope("swap1"):
        first_swap.wait()
    send_e[...] = (
        (halves[core].astype(jnp.float32) + half_in[...].astype(jnp.float32))
        .astype(bf16)
        .reshape(send_e.shape)
    )
    move_e.start()
    recv_e[within] = send_e[within]
    move_d(groups - 1, 0).start()
    for g in range(groups):
        with jax.named_scope(f"wait_c{g}"):
            move_c(g).arrived()
        for h in range(rows):
            inverse_row(h, g, tok, inv_mix, recv_c, mixed)

    with jax.named_scope("wait_e"):
        move_e.arrived()
    send_f[...] = jnp.sum(recv_e[...].astype(jnp.float32), axis=0).astype(bf16)
    move_f.start()
    recv_f[across] = send_f[across]
    for h in range(1, rows - 1):
        move_d(groups - 1, h).start()
    for g in range(groups):
        move_a(g).left()
        move_b(g).left()
        move_c(g).left()
    with jax.named_scope("wait_f"):
        move_f.arrived()
    total = jnp.sum(recv_f[...].astype(jnp.float32), axis=0) * (1.0 / divisor)
    in_bias_grad[...] = total[per : per + 2]
    out_bias_grad[...] = total[per + 2 : per + 4]
    part[...] = total.astype(bf16)
    move_g.start()
    gathered[within, across] = part[...]
    move_d(groups - 1, rows - 1).start()
    for g in range(groups - 1):
        for h in range(rows):
            with jax.named_scope(f"wait_d{g}"):
                move_d(g, h).arrived()
            inverse_row(h, g, cot, inv_grad, recv_d, grad)
    with jax.named_scope("wait_g"):
        move_g.arrived()
    move_h.start()
    for h in range(rows - 1):
        with jax.named_scope(f"wait_dl{h}"):
            move_d(groups - 1, h).arrived()
        inverse_row(h, groups - 1, cot, inv_grad, recv_d, grad)
    with jax.named_scope("wait_h"):
        move_h.arrived()
    last_swap = swap(1, gathered, other)
    last_swap.start()
    both[core] = gathered[...].reshape(n * 16, channels)
    for move in (move_e, move_f, move_g, move_h):
        move.left()
    for g in range(groups - 1):
        for h in range(rows):
            move_d(g, h).left()
    with jax.named_scope("wait_dl2"):
        move_d(groups - 1, rows - 1).arrived()
    inverse_row(rows - 1, groups - 1, cot, inv_grad, recv_d, grad)
    with jax.named_scope("swap2"):
        last_swap.wait()
    both[partner] = other[...].reshape(n * 16, channels)
    to_row = lax.broadcasted_iota(jnp.int32, (2 * BLOCK, n * 16), 0)
    from_row = lax.broadcasted_iota(jnp.int32, (2 * BLOCK, n * 16), 1)
    order = (to_row // per * 16 + to_row % per == from_row).astype(bf16)
    with jax.named_scope("params"):
        for k, out in enumerate((in_weight_grad, out_weight_grad)):
            for g in range(groups):
                ordered = dot(order, both[k, :, g * GROUP : (g + 1) * GROUP]).astype(bf16)
                for i in range(PER_GROUP):
                    place = (lane_at == row_at + i * BLOCK).astype(bf16)
                    block = dot(ordered, place, (1, 1))
                    for c in range(2):
                        out[c, g * PER_GROUP + i] = block[c * BLOCK : (c + 1) * BLOCK]
    with jax.named_scope("end"):
        for h in range(rows):
            move_d(groups - 1, h).left()


def settle(*refs):
    count = len(refs) // 2
    near, far, sems = refs[:count], refs[count:-1], refs[-1]
    copies = [
        pltpu.make_async_copy(a, b, sems.at[i]) for i, (a, b) in enumerate(zip(near, far))
    ]
    for copy in copies:
        copy.start()
    for copy in copies:
        copy.wait()


def fits(n, reps, samples, rows, channels):
    per_row = samples * (MODES // n) * 2
    return (
        reps == 2
        and MODES % n == 0
        and per_row % 16 == 0
        and channels % GROUP == 0
        and channels == BLOCKS * BLOCK
        and (4 * BLOCK) % (2 * n) == 0
        and n > 3
        and n & (n - 1) == 0
        and rows > 1
        and 4 * BLOCK // (2 * n) + 4 <= 16
        and (samples * MODES // n * rows * n) % 16 == 0
    )


def shards(tokens, cotangent, in_weight, in_bias, out_weight, out_bias):
    samples, rows, width, channels = tokens.shape
    n, reps = lax.axis_size("seq"), lax.axis_size("rep")
    if not fits(n, reps, samples, rows, channels):
        return shards_plain(tokens, cotangent, in_weight, in_bias, out_weight, out_bias)
    length = rows * n
    inner = 2 ** ((n.bit_length() - 1) // 2)
    outer = n // inner
    chunk = rows * samples * (MODES // n) * 2
    whole = n * chunk
    groups = channels // GROUP
    tables = [jnp.asarray(t) for t in kernel_tables(width, length, n, samples, rows)]
    bf16, f32 = jnp.bfloat16, jnp.float32
    block = pltpu.VMEM((groups, n, chunk, GROUP), bf16)
    small = pltpu.VMEM((n, 16, channels), bf16)
    ringed = pltpu.VMEM((inner, outer, 16, channels), bf16)
    lined = pltpu.VMEM((outer, 16, channels), bf16)
    planes = (tokens.transpose(1, 2, 0, 3), cotangent.transpose(1, 2, 0, 3))
    kept = pltpu.VMEM((groups, whole, GROUP), bf16)
    anywhere = pl.BlockSpec(memory_space=pl.ANY)
    far = pl.BlockSpec(memory_space=pltpu.HBM)
    inputs = (*planes, *tables, in_weight, in_bias, out_weight, out_bias)
    shapes = (
        (planes[0].shape, bf16),
        (planes[1].shape, bf16),
        (in_weight.shape, f32),
        (in_bias.shape, f32),
        (out_weight.shape, f32),
        (out_bias.shape, f32),
    )
    near = pl.pallas_call(
        functools.partial(mixer, n, inner, float(samples * reps)),
        out_shape=tuple(pltpu.VMEM(*shape) for shape in shapes),
        in_specs=[far] * 11,
        grid=(1,),
        out_specs=(pl.BlockSpec(memory_space=pltpu.VMEM),) * 6,
        scratch_shapes=[pltpu.VMEM(v.shape, v.dtype) for v in inputs]
        + [block] * 8
        + [ringed, lined] * 2
        + [
            pltpu.VMEM((whole, whole), bf16),
            pltpu.VMEM((4, groups, GROUP, GROUP), bf16),
            kept,
            kept,
            pltpu.VMEM((groups, whole, GROUP), f32),
            kept,
            kept,
            pltpu.VMEM((whole, GROUP), bf16),
            pltpu.VMEM((4 * BLOCK + 16, channels), bf16),
            pltpu.VMEM((2, n, 16, channels), bf16),
            small,
            pltpu.VMEM((16, channels), bf16),
            ringed,
            ringed,
            pltpu.VMEM((2, n * 16, channels), bf16),
            pltpu.SemaphoreType.DMA(((3 + rows) * groups + 4,)),
            pltpu.SemaphoreType.DMA(((3 + rows) * groups + 4,)),
            pltpu.SemaphoreType.DMA((2,)),
            pltpu.SemaphoreType.DMA((2,)),
            pltpu.SemaphoreType.DMA((2 * rows + 9,)),
        ],
        compiler_params=pltpu.CompilerParams(
            collective_id=0, has_side_effects=True, vmem_limit_bytes=VMEM_LIMIT
        ),
        name="mixer",
    )(*inputs)
    mixed, grad, *parameter_grads = pl.pallas_call(
        settle,
        out_shape=tuple(jax.ShapeDtypeStruct(*shape) for shape in shapes),
        in_specs=[anywhere] * 6,
        out_specs=(far,) * 6,
        scratch_shapes=[pltpu.SemaphoreType.DMA((6,))],
        compiler_params=pltpu.CompilerParams(vmem_limit_bytes=1 << 20),
        name="settle",
    )(*(pltpu.with_memory_space_constraint(part, pltpu.VMEM) for part in near))
    return (
        mixed.transpose(2, 0, 1, 3),
        grad.transpose(2, 0, 1, 3),
        *parameter_grads,
    )


def solution(mesh):
    in_specs = (P("rep", "seq", None, None), P("rep", "seq", None, None), P(), P(), P(), P())
    out_specs = (P("rep", "seq", None, None), P("rep", "seq", None, None), P(), P(), P(), P())
    return jax.shard_map(shards, mesh=mesh, in_specs=in_specs, out_specs=out_specs, check_vma=False)
```

```python
import functools
import math

import jax
import jax.numpy as jnp
import ml_dtypes
import numpy as np
from jax import lax
from jax.experimental import pallas as pl
from jax.experimental.pallas import tpu as pltpu
from jax.sharding import PartitionSpec as P

BLOCKS = 8
BLOCK = 96
MODES = 64


def grid_tables(length, modes):
    position = jnp.arange(length, dtype=jnp.int32)
    frequency = jnp.arange(modes, dtype=jnp.int32)
    residue = position[:, None] * frequency[None, :] % length
    angles = residue.astype(jnp.float32) * (2.0 * math.pi / length)
    factor = 1.0 / math.sqrt(length)
    cosine_table = (jnp.cos(angles) * factor).astype(jnp.bfloat16)
    sine_table = (jnp.sin(angles) * factor).astype(jnp.bfloat16)
    return (cosine_table, sine_table)


def column_tables(grid_width, modes):
    cosine_table, sine_table = grid_tables(grid_width, modes)
    forward = jnp.stack([cosine_table, -sine_table], axis=2)
    doubling = jnp.where(jnp.arange(modes) == 0, 1.0, 2.0).astype(jnp.bfloat16)[:, None]
    inverse = jnp.stack([cosine_table.T * doubling, -(sine_table.T * doubling)], axis=1)
    return (forward, inverse)


def row_table(length):
    cosine_table, sine_table = grid_tables(length, length)
    upper_rows = jnp.stack([cosine_table, sine_table], axis=2)
    lower_rows = jnp.stack([-sine_table, cosine_table], axis=2)
    return jnp.stack([upper_rows, lower_rows], axis=1)


def block_weights(weight):
    real_part, imag_part = (weight[0], weight[1])
    upper_half = jnp.stack([real_part, imag_part], axis=2)
    lower_half = jnp.stack([-imag_part, real_part], axis=2)
    return jnp.stack([upper_half, lower_half], axis=1)


def fold_blocks(blockwise):
    real_part = blockwise[:, 0, :, 0, :] + blockwise[:, 1, :, 1, :]
    imag_part = blockwise[:, 0, :, 1, :] - blockwise[:, 1, :, 0, :]
    return jnp.stack([real_part, imag_part])


def mix_forward(spectrum, weights_in, weights_out, bias_in, bias_out):
    mode_count = spectrum.shape[0] * spectrum.shape[1] * spectrum.shape[2]
    flat_modes = spectrum.reshape(mode_count, 2, BLOCKS, BLOCK)
    hidden_pre = (
        jnp.einsum("mcbi,bciej->mebj", flat_modes, weights_in, preferred_element_type=jnp.float32)
        + bias_in
    )
    hidden = jax.nn.gelu(hidden_pre).astype(jnp.bfloat16)
    spectrum_out = (
        jnp.einsum("mcbi,bciej->mebj", hidden, weights_out, preferred_element_type=jnp.float32)
        + bias_out
    )
    return (
        flat_modes,
        hidden_pre,
        hidden,
        spectrum_out.astype(jnp.bfloat16).reshape(spectrum.shape),
    )


def mix_backward(flat_modes, hidden_pre, hidden, incoming, weights_in, weights_out):
    incoming_flat = incoming.reshape(flat_modes.shape)
    out_bias_part = jnp.sum(incoming_flat.astype(jnp.float32), axis=0).reshape(2, -1)
    out_weight_part = fold_blocks(
        jnp.einsum("mcbi,mebj->bciej", hidden, incoming_flat, preferred_element_type=jnp.float32)
    )
    hidden_grad = jnp.einsum(
        "mebj,bciej->mcbi", incoming_flat, weights_out, preferred_element_type=jnp.float32
    )
    pre_grad = jax.vjp(jax.nn.gelu, hidden_pre)[1](hidden_grad)[0].astype(jnp.bfloat16)
    in_bias_part = jnp.sum(pre_grad.astype(jnp.float32), axis=0).reshape(2, -1)
    in_weight_part = fold_blocks(
        jnp.einsum("mcbi,mebj->bciej", flat_modes, pre_grad, preferred_element_type=jnp.float32)
    )
    spectrum_grad = jnp.einsum(
        "mebj,bciej->mcbi", pre_grad, weights_in, preferred_element_type=jnp.float32
    )
    spectrum_grad = spectrum_grad.astype(jnp.bfloat16).reshape(incoming.shape)
    return (spectrum_grad, (in_weight_part, in_bias_part, out_weight_part, out_bias_part))


def shards_plain(tokens, cotangent, in_weight, in_bias, out_weight, out_bias):
    samples, row_count, grid_width, channels = tokens.shape
    length = row_count * lax.axis_size("seq")
    column_forward, column_inverse = column_tables(grid_width, MODES)
    row_matrix = row_table(length)
    weights_in = block_weights(in_weight)
    weights_out = block_weights(out_weight)
    bias_in = in_bias.reshape(2, BLOCKS, BLOCK)
    bias_out = out_bias.reshape(2, BLOCKS, BLOCK)

    def along_rows(section):
        return jnp.einsum(
            "qehc,shkcd->sqked", row_matrix, section, preferred_element_type=jnp.float32
        ).astype(jnp.bfloat16)

    def back_rows(section):
        return jnp.einsum(
            "qehc,sqked->shkcd", row_matrix, section, preferred_element_type=jnp.float32
        ).astype(jnp.bfloat16)

    spec_rows = jnp.einsum(
        "shwd,wkc->shkcd", tokens, column_forward, preferred_element_type=jnp.float32
    ).astype(jnp.bfloat16)
    spectrum = along_rows(lax.all_to_all(spec_rows, "seq", split_axis=2, concat_axis=1, tiled=True))
    flat_modes, hidden_pre, hidden, spectrum_out = mix_forward(
        spectrum, weights_in, weights_out, bias_in, bias_out
    )
    mixed_grid = jnp.einsum(
        "shkcd,kcw->shwd",
        lax.all_to_all(back_rows(spectrum_out), "seq", split_axis=1, concat_axis=2, tiled=True),
        column_inverse,
        preferred_element_type=jnp.float32,
    )
    cot_rows = jnp.einsum(
        "shwd,kcw->shkcd", cotangent, column_inverse, preferred_element_type=jnp.float32
    ).astype(jnp.bfloat16)
    incoming = along_rows(lax.all_to_all(cot_rows, "seq", split_axis=2, concat_axis=1, tiled=True))
    spectrum_grad, partials = mix_backward(
        flat_modes, hidden_pre, hidden, incoming, weights_in, weights_out
    )
    adjoint_part = jnp.einsum(
        "shkcd,wkc->shwd",
        lax.all_to_all(back_rows(spectrum_grad), "seq", split_axis=1, concat_axis=2, tiled=True),
        column_forward,
        preferred_element_type=jnp.float32,
    )
    mixed_out = (tokens.astype(jnp.float32) + mixed_grid).astype(jnp.bfloat16)
    tokens_grad = (cotangent.astype(jnp.float32) + adjoint_part).astype(jnp.bfloat16)
    totals = lax.psum((partials[0], partials[1], partials[2], partials[3]), ("seq", "rep"))
    divisor = float(samples * lax.axis_size("rep"))
    return (
        mixed_out,
        tokens_grad,
        totals[0] / divisor,
        totals[1] / divisor,
        totals[2] / divisor,
        totals[3] / divisor,
    )


GROUP = math.lcm(BLOCK, 128)
PER_GROUP = GROUP // BLOCK
MESH_ID = pl.DeviceIdType.MESH
VMEM_LIMIT = 52 << 20
FIRST, AFTER_E, AFTER_F, AFTER_G = 2, 1, 2, 1


def host_tables(length, modes):
    residue = np.arange(length)[:, None] * np.arange(modes)[None, :] % length
    angles = residue.astype(np.float32) * np.float32(2.0 * math.pi / length)
    factor = np.float32(1.0 / math.sqrt(length))
    rounded = [(f(angles) * factor).astype(ml_dtypes.bfloat16) for f in (np.cos, np.sin)]
    return [table.astype(np.float32) for table in rounded]


def kernel_tables(width, length, n, samples, rows):
    local = MODES // n
    cosine, sine = host_tables(width, MODES)
    forward = np.stack([cosine.T, -sine.T], axis=1)
    doubled = forward * np.where(np.arange(MODES) == 0, 1.0, 2.0)[:, None, None]

    def spread(table):
        table = table.reshape(n, local, 2, width)
        whole = np.zeros((n, samples, local, 2, width, samples), np.float32)
        for s in range(samples):
            whole[:, s, :, :, :, s] = table
        return whole.reshape(n * samples * local * 2, width * samples)

    cosine, sine = host_tables(length, length)
    upper = np.stack([cosine, sine], axis=2)
    lower = np.stack([-sine, cosine], axis=2)
    turn = np.stack([upper, lower], axis=0)
    both = samples * local
    mixing = np.zeros((2, both, length, length, both, 2), np.float32)
    for x in range(both):
        mixing[:, x, :, :, x, :] = turn
    mixing = mixing.reshape(2 * both * length, length * both * 2)

    flat = [
        spread(forward),
        spread(doubled),
        spread(doubled).T,
        spread(forward).T,
        mixing,
    ]
    return [np.ascontiguousarray(t).astype(ml_dtypes.bfloat16) for t in flat]


def dot(a, b, contract=(1, 0)):
    return lax.dot_general(
        a, b, (((contract[0],), (contract[1],)), ((), ())), preferred_element_type=jnp.float32
    )


def mixer(
    n,
    inner,
    divisor,
    tok_far,
    cot_far,
    col_tok_far,
    col_cot_far,
    inv_mix_far,
    inv_grad_far,
    turn_far,
    in_weight_far,
    in_bias_far,
    out_weight_far,
    out_bias_far,
    mixed,
    grad,
    in_weight_grad,
    in_bias_grad,
    out_weight_grad,
    out_bias_grad,
    tok,
    cot,
    col_tok,
    col_cot,
    inv_mix,
    inv_grad,
    turn,
    in_weight,
    in_bias,
    out_weight,
    out_bias,
    send_a,
    send_b,
    send_c,
    send_d,
    recv_a,
    recv_b,
    recv_c,
    recv_d,
    send_e,
    send_f,
    recv_e,
    recv_f,
    turn_back,
    wide,
    spec,
    hid,
    slope,
    inc,
    pre,
    mixed_modes,
    grads,
    halves,
    half_in,
    part,
    gathered,
    other,
    both,
    send_sem,
    recv_sem,
    pair_send,
    pair_recv,
    load_sem,
):
    me = lax.axis_index("seq")
    core = lax.axis_index("rep")
    partner = 1 - core
    rows, width, samples, channels = tok.shape
    groups = channels // GROUP
    outer = n // inner
    across, within = me // inner, lax.rem(me, inner)
    chunk = send_a.shape[2]
    row_chunk = chunk // rows
    bf16 = jnp.bfloat16

    barrier = pltpu.get_barrier_semaphore()

    def greet(j, carry):
        peer = lax.rem(me + j, n)
        pl.semaphore_signal(barrier, inc=1, device_id={"seq": peer}, device_id_type=MESH_ID)
        return carry

    lax.fori_loop(1, n, greet, 0)
    pl.semaphore_signal(barrier, inc=1, device_id={"rep": partner}, device_id_type=MESH_ID)

    moves = [(col_tok_far, col_tok)]
    moves += [(tok_far.at[h], tok.at[h]) for h in range(rows)]
    moves += [(col_cot_far, col_cot)]
    moves += [(cot_far.at[h], cot.at[h]) for h in range(rows)]
    moves += [
        (in_weight_far, in_weight),
        (out_weight_far, out_weight),
        (turn_far, turn),
        (in_bias_far, in_bias),
        (out_bias_far, out_bias),
        (inv_mix_far, inv_mix),
        (inv_grad_far, inv_grad),
    ]
    loads = [
        pltpu.make_async_copy(far, near, load_sem.at[i]) for i, (far, near) in enumerate(moves)
    ]
    for load in loads[: rows + 1]:
        load.start()

    def copy_to(slot, peer, source, target):
        return pltpu.make_async_remote_copy(
            src_ref=source,
            dst_ref=target,
            send_sem=send_sem.at[slot],
            recv_sem=recv_sem.at[slot],
            device_id={"seq": peer},
            device_id_type=MESH_ID,
        )

    def loop(count, act):
        def step(j, carry):
            act(j)
            return carry

        lax.fori_loop(1, count, step, 0)

    def peer_at(j):
        peer = jnp.int32(0)
        bit = 1
        while bit < n:
            peer = peer + bit * lax.rem(me // bit + j // bit, 2)
            bit *= 2
        return peer

    class Move:
        def __init__(self, slot, count, to, source, target, span):
            self.slot, self.count, self.to = slot, count, to
            self.source, self.target, self.span = source, target, span

        def start(self):
            def out(j):
                at, peer = self.to(j)
                copy_to(self.slot, peer, self.source(at), self.target).start()

            loop(self.count, out)

        def all(self):
            return copy_to(self.slot, me, self.span, self.span)

        def arrived(self):
            self.all().wait_recv()

        def left(self):
            self.all().wait_send()

    def to_peer(j):
        peer = peer_at(j)
        return peer, peer

    def to_plane(j):
        v = lax.rem(within + j, inner)
        return v, across * inner + v

    def to_line(j):
        z = lax.rem(across + j, outer)
        return z, z * inner + within

    def everyone(slot, source, target, g, at=None):
        cut = pl.ds(0, chunk) if at is None else at
        return Move(
            slot,
            n,
            to_peer,
            lambda peer: source.at[g, peer, cut],
            target.at[g, me, cut],
            target.at[g, pl.ds(0, n - 1), cut],
        )

    def move_a(g):
        return everyone(g, send_a, recv_a, g)

    def move_b(g):
        return everyone(groups + g, send_b, recv_b, g)

    def move_c(g, h):
        at = pl.ds(h * row_chunk, row_chunk)
        return everyone(2 * groups + g * rows + h, send_c, recv_c, g, at)

    def move_d(g, h):
        at = pl.ds(h * row_chunk, row_chunk)
        return everyone((2 + rows) * groups + g * rows + h, send_d, recv_d, g, at)

    tail = (2 + 2 * rows) * groups
    move_e = Move(
        tail,
        inner,
        to_plane,
        lambda v: send_e.at[v],
        recv_e.at[within],
        recv_e.at[pl.ds(0, inner - 1)],
    )
    move_f = Move(
        tail + 1,
        outer,
        to_line,
        lambda z: send_f.at[z],
        recv_f.at[across],
        recv_f.at[pl.ds(0, outer - 1)],
    )
    move_g = Move(
        tail + 2,
        outer,
        to_line,
        lambda z: part,
        gathered.at[within, across],
        gathered.at[within, pl.ds(0, outer - 1)],
    )
    move_h = Move(
        tail + 3,
        inner,
        to_plane,
        lambda v: gathered.at[within],
        gathered.at[within],
        gathered.at[pl.ds(0, inner - 1)],
    )

    def lanes(g):
        return pl.ds(pl.multiple_of(g * GROUP, GROUP), GROUP)

    def fixed(g):
        return pl.ds(g * GROUP, GROUP)

    def columns(tokens, table, send, g):
        for h in range(rows):
            section = tokens[h, :, :, fixed(g)].reshape(width * samples, GROUP)
            send[g, :, h * row_chunk : (h + 1) * row_chunk, :] = (
                dot(table[...], section).astype(bf16).reshape(n, row_chunk, GROUP)
            )

    for load in loads[: rows + 1]:
        load.wait()
    for load in loads[rows + 1 :]:
        load.start()
    for g in range(groups):
        columns(tok, col_tok, send_a, g)
        if g == 0:
            pl.semaphore_wait(barrier, n)
        move_a(g).start()
        if g == 0:
            for load in loads[rows + 1 : 2 * rows + 2]:
                load.wait()
        columns(cot, col_cot, send_b, g)
        move_b(g).start()
    for load in loads[2 * rows + 2 :]:
        load.wait()
    recv_a[:, me] = send_a[:, me]
    recv_b[:, me] = send_b[:, me]

    turn_back[...] = turn[...].T
    row_at = lax.broadcasted_iota(jnp.int32, (BLOCK, GROUP), 0)
    lane_at = lax.broadcasted_iota(jnp.int32, (BLOCK, GROUP), 1)
    for at, weight in enumerate((in_weight, out_weight)):
        for i in range(PER_GROUP):
            place = (lane_at == row_at + i * BLOCK).astype(bf16)
            for c in range(2):
                for g in range(groups):
                    wide[2 * at + c, g, i * BLOCK : (i + 1) * BLOCK, :] = dot(
                        weight[c, g * PER_GROUP + i], place
                    ).astype(bf16)

    half = turn.shape[0] // 2
    scale = math.sqrt(2.0 / math.pi)

    def per_group(act):
        def step(g, carry):
            act(g, lanes(g))
            return carry

        lax.fori_loop(0, groups, step, 0)

    def along_rows(recv, keep, g):
        keep[g] = dot(turn[...], recv[g].reshape(turn.shape[1], GROUP)).astype(bf16)

    def back_rows(send, g):
        send[g] = dot(turn_back[...], mixed_modes[...]).astype(bf16).reshape(n, chunk, GROUP)

    def forward_group(g, at):
        along_rows(recv_a, spec, g)
        re, im = spec[g, :half], spec[g, half:]
        w_re, w_im = wide[0, g], wide[1, g]
        for c in range(2):
            if c == 0:
                value = dot(re, w_re) - dot(im, w_im)
            else:
                value = dot(re, w_im) + dot(im, w_re)
            value = value + in_bias[c : c + 1, at]
            square = value * value
            tanh = jnp.tanh(scale * value * (1.0 + 0.044715 * square))
            hid[g, c * half : (c + 1) * half] = (0.5 * value * (1.0 + tanh)).astype(bf16)
            slope[g, c * half : (c + 1) * half] = 0.5 * (1.0 + tanh) + 0.5 * value * (
                1.0 - tanh * tanh
            ) * (scale * (1.0 + (3.0 * 0.044715) * square))
        re, im = hid[g, :half], hid[g, half:]
        w_re, w_im = wide[2, g], wide[3, g]
        mixed_modes[:half] = (
            dot(re, w_re) - dot(im, w_im) + out_bias[0:1, at]
        ).astype(bf16)
        mixed_modes[half:] = (
            dot(re, w_im) + dot(im, w_re) + out_bias[1:2, at]
        ).astype(bf16)
        back_rows(send_c, g)

    def backward_group(g):
        along_rows(recv_b, inc, g)
        re, im = inc[g, :half], inc[g, half:]
        w_re, w_im = wide[2, g], wide[3, g]
        pre[g, :half] = (
            (dot(re, w_re, (1, 1)) + dot(im, w_im, (1, 1))) * slope[g, :half]
        ).astype(bf16)
        pre[g, half:] = (
            (dot(im, w_re, (1, 1)) - dot(re, w_im, (1, 1))) * slope[g, half:]
        ).astype(bf16)
        re, im = pre[g, :half], pre[g, half:]
        w_re, w_im = wide[0, g], wide[1, g]
        mixed_modes[:half] = (dot(re, w_re, (1, 1)) + dot(im, w_im, (1, 1))).astype(bf16)
        mixed_modes[half:] = (dot(im, w_re, (1, 1)) - dot(re, w_im, (1, 1))).astype(bf16)
        back_rows(send_d, g)

    def fold(product):
        total = jnp.zeros((BLOCK, GROUP), jnp.float32)
        for i in range(PER_GROUP):
            inside = (lane_at >= i * BLOCK) & (lane_at < (i + 1) * BLOCK)
            total = jnp.where(inside, product[i * BLOCK : (i + 1) * BLOCK], total)
        return total.astype(bf16)

    bias_at = lax.broadcasted_iota(jnp.int32, (16, GROUP), 0)

    def grads_group(g, at):
        bias = jnp.zeros((16, GROUP), jnp.float32)
        for k, (left, right) in enumerate(((spec, pre), (hid, inc))):
            a_re, a_im = left[g, :half], left[g, half:]
            b_re, b_im = right[g, :half], right[g, half:]
            first = 2 * k * BLOCK
            grads[first : first + BLOCK, at] = fold(
                dot(a_re, b_re, (0, 0)) + dot(a_im, b_im, (0, 0))
            )
            grads[first + BLOCK : first + 2 * BLOCK, at] = fold(
                dot(a_re, b_im, (0, 0)) - dot(a_im, b_re, (0, 0))
            )
            for c, value in enumerate((b_re, b_im)):
                total = jnp.sum(value.astype(jnp.float32), axis=0, keepdims=True)
                bias = jnp.where(bias_at == 2 * k + c, total, bias)
        grads[4 * BLOCK : 4 * BLOCK + 16, at] = bias.astype(bf16)

    last = groups - 1
    held = [move_c(last, h) for h in range(rows)]
    held += [move_d(g, h) for g in range(groups) for h in range(rows)]

    def release(count):
        for move in held[:count]:
            move.start()
        del held[:count]

    def mix_group(g, at):
        with jax.named_scope("wait_a"):
            move_a(g).arrived()
        with jax.named_scope("fwd"):
            forward_group(g, at)
        recv_c[g, me] = send_c[g, me]

        @pl.when(g < last)
        def _():
            for h in range(rows):
                move_c(g, h).start()

        with jax.named_scope("wait_b"):
            move_b(g).arrived()

        @pl.when(g == last)
        def _():
            release(FIRST)

        with jax.named_scope("bwd"):
            backward_group(g)
        recv_d[g, me] = send_d[g, me]
        with jax.named_scope("grads"):
            grads_group(g, at)

    per_group(mix_group)

    per = 4 * BLOCK // (2 * n)
    to_row = lax.broadcasted_iota(jnp.int32, (2 * n * 16, 4 * BLOCK + 16), 0)
    from_row = lax.broadcasted_iota(jnp.int32, (2 * n * 16, 4 * BLOCK + 16), 1)
    slot = to_row % 16
    wanted = jnp.where(slot < per, to_row // 16 * per + slot, 4 * BLOCK + slot - per)
    picks = (wanted == from_row).astype(bf16)
    halves[...] = dot(picks, grads[...]).astype(bf16).reshape(halves.shape)

    def swap(slot, source, target):
        return pltpu.make_async_remote_copy(
            src_ref=source,
            dst_ref=target,
            send_sem=pair_send.at[slot],
            recv_sem=pair_recv.at[slot],
            device_id={"rep": partner},
            device_id_type=MESH_ID,
        )

    first_swap = swap(0, halves.at[partner], half_in)
    first_swap.start()

    def inverse_row(h, g, tokens, table, recv, out):
        section = recv[g, :, h * row_chunk : (h + 1) * row_chunk, :]
        product = dot(table[...], section.reshape(n * row_chunk, GROUP))
        kept = tokens[h, :, :, fixed(g)].reshape(width * samples, GROUP).astype(jnp.float32)
        out[h, :, :, fixed(g)] = (kept + product).astype(bf16).reshape(width, samples, GROUP)

    with jax.named_scope("swap1"):
        first_swap.wait()
    send_e[...] = (
        (halves[core].astype(jnp.float32) + half_in[...].astype(jnp.float32))
        .astype(bf16)
        .reshape(send_e.shape)
    )
    move_e.start()
    recv_e[within] = send_e[within]
    release(AFTER_E)
    with jax.named_scope("wait_e"):
        move_e.arrived()
    send_f[...] = jnp.sum(recv_e[...].astype(jnp.float32), axis=0).astype(bf16)
    move_f.start()
    recv_f[across] = send_f[across]
    release(AFTER_F)
    with jax.named_scope("wait_f"):
        move_f.arrived()
    total = jnp.sum(recv_f[...].astype(jnp.float32), axis=0) * (1.0 / divisor)
    in_bias_grad[...] = total[per : per + 2]
    out_bias_grad[...] = total[per + 2 : per + 4]
    part[...] = total.astype(bf16)
    move_g.start()
    gathered[within, across] = part[...]
    release(AFTER_G)
    with jax.named_scope("wait_g"):
        move_g.arrived()
    move_h.start()
    release(len(held))
    def finish_c(g, h):
        with jax.named_scope(f"wait_c{g}{h}"):
            move_c(g, h).arrived()
        inverse_row(h, g, tok, inv_mix, recv_c, mixed)

    def finish_d(g, h):
        with jax.named_scope(f"wait_d{g}{h}"):
            move_d(g, h).arrived()
        inverse_row(h, g, cot, inv_grad, recv_d, grad)

    for g in range(groups):
        for h in range(rows):
            finish_c(g, h)
    for g in range(groups):
        move_a(g).left()
        move_b(g).left()
    for move in (move_e, move_f, move_g):
        move.left()
    for g in range(last):
        for h in range(rows):
            finish_d(g, h)
    with jax.named_scope("wait_h"):
        move_h.arrived()
    last_swap = swap(1, gathered, other)
    last_swap.start()
    both[core] = gathered[...].reshape(n * 16, channels)
    move_h.left()
    for g in range(groups):
        for h in range(rows):
            move_c(g, h).left()
    for h in range(rows - 1):
        finish_d(last, h)
    with jax.named_scope("swap2"):
        last_swap.wait()
    both[partner] = other[...].reshape(n * 16, channels)
    to_row = lax.broadcasted_iota(jnp.int32, (2 * BLOCK, n * 16), 0)
    from_row = lax.broadcasted_iota(jnp.int32, (2 * BLOCK, n * 16), 1)
    order = (to_row // per * 16 + to_row % per == from_row).astype(bf16)
    with jax.named_scope("params"):
        for k, out in enumerate((in_weight_grad, out_weight_grad)):
            for g in range(groups):
                ordered = dot(order, both[k, :, g * GROUP : (g + 1) * GROUP]).astype(bf16)
                for i in range(PER_GROUP):
                    place = (lane_at == row_at + i * BLOCK).astype(bf16)
                    block = dot(ordered, place, (1, 1))
                    for c in range(2):
                        out[c, g * PER_GROUP + i] = block[c * BLOCK : (c + 1) * BLOCK]
    finish_d(last, rows - 1)
    with jax.named_scope("end"):
        for g in range(groups):
            for h in range(rows):
                move_d(g, h).left()


def settle(*refs):
    count = len(refs) // 2
    near, far, sems = refs[:count], refs[count:-1], refs[-1]
    copies = [
        pltpu.make_async_copy(a, b, sems.at[i]) for i, (a, b) in enumerate(zip(near, far))
    ]
    for copy in copies:
        copy.start()
    for copy in copies:
        copy.wait()


def fits(n, reps, samples, rows, channels):
    per_row = samples * (MODES // n) * 2
    return (
        reps == 2
        and MODES % n == 0
        and per_row % 16 == 0
        and channels % GROUP == 0
        and channels == BLOCKS * BLOCK
        and (4 * BLOCK) % (2 * n) == 0
        and n > 3
        and n & (n - 1) == 0
        and rows > 1
        and 4 * BLOCK // (2 * n) + 4 <= 16
        and (samples * MODES // n * rows * n) % 16 == 0
    )


def shards(tokens, cotangent, in_weight, in_bias, out_weight, out_bias):
    samples, rows, width, channels = tokens.shape
    n, reps = lax.axis_size("seq"), lax.axis_size("rep")
    if not fits(n, reps, samples, rows, channels):
        return shards_plain(tokens, cotangent, in_weight, in_bias, out_weight, out_bias)
    length = rows * n
    inner = 2 ** ((n.bit_length() - 1) // 2)
    outer = n // inner
    chunk = rows * samples * (MODES // n) * 2
    whole = n * chunk
    groups = channels // GROUP
    tables = [jnp.asarray(t) for t in kernel_tables(width, length, n, samples, rows)]
    bf16, f32 = jnp.bfloat16, jnp.float32
    block = pltpu.VMEM((groups, n, chunk, GROUP), bf16)
    small = pltpu.VMEM((n, 16, channels), bf16)
    ringed = pltpu.VMEM((inner, outer, 16, channels), bf16)
    lined = pltpu.VMEM((outer, 16, channels), bf16)
    planes = (tokens.transpose(1, 2, 0, 3), cotangent.transpose(1, 2, 0, 3))
    kept = pltpu.VMEM((groups, whole, GROUP), bf16)
    anywhere = pl.BlockSpec(memory_space=pl.ANY)
    far = pl.BlockSpec(memory_space=pltpu.HBM)
    inputs = (*planes, *tables, in_weight, in_bias, out_weight, out_bias)
    shapes = (
        (planes[0].shape, bf16),
        (planes[1].shape, bf16),
        (in_weight.shape, f32),
        (in_bias.shape, f32),
        (out_weight.shape, f32),
        (out_bias.shape, f32),
    )
    near = pl.pallas_call(
        functools.partial(mixer, n, inner, float(samples * reps)),
        out_shape=tuple(pltpu.VMEM(*shape) for shape in shapes),
        in_specs=[far] * 11,
        grid=(1,),
        out_specs=(pl.BlockSpec(memory_space=pltpu.VMEM),) * 6,
        scratch_shapes=[pltpu.VMEM(v.shape, v.dtype) for v in inputs]
        + [block] * 8
        + [ringed, lined] * 2
        + [
            pltpu.VMEM((whole, whole), bf16),
            pltpu.VMEM((4, groups, GROUP, GROUP), bf16),
            kept,
            kept,
            pltpu.VMEM((groups, whole, GROUP), f32),
            kept,
            kept,
            pltpu.VMEM((whole, GROUP), bf16),
            pltpu.VMEM((4 * BLOCK + 16, channels), bf16),
            pltpu.VMEM((2, n, 16, channels), bf16),
            small,
            pltpu.VMEM((16, channels), bf16),
            ringed,
            ringed,
            pltpu.VMEM((2, n * 16, channels), bf16),
            pltpu.SemaphoreType.DMA(((2 + 2 * rows) * groups + 4,)),
            pltpu.SemaphoreType.DMA(((2 + 2 * rows) * groups + 4,)),
            pltpu.SemaphoreType.DMA((2,)),
            pltpu.SemaphoreType.DMA((2,)),
            pltpu.SemaphoreType.DMA((2 * rows + 9,)),
        ],
        compiler_params=pltpu.CompilerParams(
            collective_id=0, has_side_effects=True, vmem_limit_bytes=VMEM_LIMIT
        ),
        name="mixer",
    )(*inputs)
    mixed, grad, *parameter_grads = pl.pallas_call(
        settle,
        out_shape=tuple(jax.ShapeDtypeStruct(*shape) for shape in shapes),
        in_specs=[anywhere] * 6,
        out_specs=(far,) * 6,
        scratch_shapes=[pltpu.SemaphoreType.DMA((6,))],
        compiler_params=pltpu.CompilerParams(vmem_limit_bytes=1 << 20),
        name="settle",
    )(*(pltpu.with_memory_space_constraint(part, pltpu.VMEM) for part in near))
    return (
        mixed.transpose(2, 0, 1, 3),
        grad.transpose(2, 0, 1, 3),
        *parameter_grads,
    )


def solution(mesh):
    in_specs = (P("rep", "seq", None, None), P("rep", "seq", None, None), P(), P(), P(), P())
    out_specs = (P("rep", "seq", None, None), P("rep", "seq", None, None), P(), P(), P(), P())
    return jax.shard_map(shards, mesh=mesh, in_specs=in_specs, out_specs=out_specs, check_vma=False)
```

```python
import functools
import math

import jax
import jax.numpy as jnp
import ml_dtypes
import numpy as np
from jax import lax
from jax.experimental import pallas as pl
from jax.experimental.pallas import tpu as pltpu
from jax.sharding import PartitionSpec as P

BLOCKS = 8
BLOCK = 96
MODES = 64


def grid_tables(length, modes):
    position = jnp.arange(length, dtype=jnp.int32)
    frequency = jnp.arange(modes, dtype=jnp.int32)
    residue = position[:, None] * frequency[None, :] % length
    angles = residue.astype(jnp.float32) * (2.0 * math.pi / length)
    factor = 1.0 / math.sqrt(length)
    cosine_table = (jnp.cos(angles) * factor).astype(jnp.bfloat16)
    sine_table = (jnp.sin(angles) * factor).astype(jnp.bfloat16)
    return (cosine_table, sine_table)


def column_tables(grid_width, modes):
    cosine_table, sine_table = grid_tables(grid_width, modes)
    forward = jnp.stack([cosine_table, -sine_table], axis=2)
    doubling = jnp.where(jnp.arange(modes) == 0, 1.0, 2.0).astype(jnp.bfloat16)[:, None]
    inverse = jnp.stack([cosine_table.T * doubling, -(sine_table.T * doubling)], axis=1)
    return (forward, inverse)


def row_table(length):
    cosine_table, sine_table = grid_tables(length, length)
    upper_rows = jnp.stack([cosine_table, sine_table], axis=2)
    lower_rows = jnp.stack([-sine_table, cosine_table], axis=2)
    return jnp.stack([upper_rows, lower_rows], axis=1)


def block_weights(weight):
    real_part, imag_part = (weight[0], weight[1])
    upper_half = jnp.stack([real_part, imag_part], axis=2)
    lower_half = jnp.stack([-imag_part, real_part], axis=2)
    return jnp.stack([upper_half, lower_half], axis=1)


def fold_blocks(blockwise):
    real_part = blockwise[:, 0, :, 0, :] + blockwise[:, 1, :, 1, :]
    imag_part = blockwise[:, 0, :, 1, :] - blockwise[:, 1, :, 0, :]
    return jnp.stack([real_part, imag_part])


def mix_forward(spectrum, weights_in, weights_out, bias_in, bias_out):
    mode_count = spectrum.shape[0] * spectrum.shape[1] * spectrum.shape[2]
    flat_modes = spectrum.reshape(mode_count, 2, BLOCKS, BLOCK)
    hidden_pre = (
        jnp.einsum("mcbi,bciej->mebj", flat_modes, weights_in, preferred_element_type=jnp.float32)
        + bias_in
    )
    hidden = jax.nn.gelu(hidden_pre).astype(jnp.bfloat16)
    spectrum_out = (
        jnp.einsum("mcbi,bciej->mebj", hidden, weights_out, preferred_element_type=jnp.float32)
        + bias_out
    )
    return (
        flat_modes,
        hidden_pre,
        hidden,
        spectrum_out.astype(jnp.bfloat16).reshape(spectrum.shape),
    )


def mix_backward(flat_modes, hidden_pre, hidden, incoming, weights_in, weights_out):
    incoming_flat = incoming.reshape(flat_modes.shape)
    out_bias_part = jnp.sum(incoming_flat.astype(jnp.float32), axis=0).reshape(2, -1)
    out_weight_part = fold_blocks(
        jnp.einsum("mcbi,mebj->bciej", hidden, incoming_flat, preferred_element_type=jnp.float32)
    )
    hidden_grad = jnp.einsum(
        "mebj,bciej->mcbi", incoming_flat, weights_out, preferred_element_type=jnp.float32
    )
    pre_grad = jax.vjp(jax.nn.gelu, hidden_pre)[1](hidden_grad)[0].astype(jnp.bfloat16)
    in_bias_part = jnp.sum(pre_grad.astype(jnp.float32), axis=0).reshape(2, -1)
    in_weight_part = fold_blocks(
        jnp.einsum("mcbi,mebj->bciej", flat_modes, pre_grad, preferred_element_type=jnp.float32)
    )
    spectrum_grad = jnp.einsum(
        "mebj,bciej->mcbi", pre_grad, weights_in, preferred_element_type=jnp.float32
    )
    spectrum_grad = spectrum_grad.astype(jnp.bfloat16).reshape(incoming.shape)
    return (spectrum_grad, (in_weight_part, in_bias_part, out_weight_part, out_bias_part))


def shards_plain(tokens, cotangent, in_weight, in_bias, out_weight, out_bias):
    samples, row_count, grid_width, channels = tokens.shape
    length = row_count * lax.axis_size("seq")
    column_forward, column_inverse = column_tables(grid_width, MODES)
    row_matrix = row_table(length)
    weights_in = block_weights(in_weight)
    weights_out = block_weights(out_weight)
    bias_in = in_bias.reshape(2, BLOCKS, BLOCK)
    bias_out = out_bias.reshape(2, BLOCKS, BLOCK)

    def along_rows(section):
        return jnp.einsum(
            "qehc,shkcd->sqked", row_matrix, section, preferred_element_type=jnp.float32
        ).astype(jnp.bfloat16)

    def back_rows(section):
        return jnp.einsum(
            "qehc,sqked->shkcd", row_matrix, section, preferred_element_type=jnp.float32
        ).astype(jnp.bfloat16)

    spec_rows = jnp.einsum(
        "shwd,wkc->shkcd", tokens, column_forward, preferred_element_type=jnp.float32
    ).astype(jnp.bfloat16)
    spectrum = along_rows(lax.all_to_all(spec_rows, "seq", split_axis=2, concat_axis=1, tiled=True))
    flat_modes, hidden_pre, hidden, spectrum_out = mix_forward(
        spectrum, weights_in, weights_out, bias_in, bias_out
    )
    mixed_grid = jnp.einsum(
        "shkcd,kcw->shwd",
        lax.all_to_all(back_rows(spectrum_out), "seq", split_axis=1, concat_axis=2, tiled=True),
        column_inverse,
        preferred_element_type=jnp.float32,
    )
    cot_rows = jnp.einsum(
        "shwd,kcw->shkcd", cotangent, column_inverse, preferred_element_type=jnp.float32
    ).astype(jnp.bfloat16)
    incoming = along_rows(lax.all_to_all(cot_rows, "seq", split_axis=2, concat_axis=1, tiled=True))
    spectrum_grad, partials = mix_backward(
        flat_modes, hidden_pre, hidden, incoming, weights_in, weights_out
    )
    adjoint_part = jnp.einsum(
        "shkcd,wkc->shwd",
        lax.all_to_all(back_rows(spectrum_grad), "seq", split_axis=1, concat_axis=2, tiled=True),
        column_forward,
        preferred_element_type=jnp.float32,
    )
    mixed_out = (tokens.astype(jnp.float32) + mixed_grid).astype(jnp.bfloat16)
    tokens_grad = (cotangent.astype(jnp.float32) + adjoint_part).astype(jnp.bfloat16)
    totals = lax.psum((partials[0], partials[1], partials[2], partials[3]), ("seq", "rep"))
    divisor = float(samples * lax.axis_size("rep"))
    return (
        mixed_out,
        tokens_grad,
        totals[0] / divisor,
        totals[1] / divisor,
        totals[2] / divisor,
        totals[3] / divisor,
    )


GROUP = math.lcm(BLOCK, 128)
PER_GROUP = GROUP // BLOCK
MESH_ID = pl.DeviceIdType.MESH
VMEM_LIMIT = 52 << 20
FIRST, AFTER_E, AFTER_F = 2, 3, 2


def host_tables(length, modes):
    residue = np.arange(length)[:, None] * np.arange(modes)[None, :] % length
    angles = residue.astype(np.float32) * np.float32(2.0 * math.pi / length)
    factor = np.float32(1.0 / math.sqrt(length))
    rounded = [(f(angles) * factor).astype(ml_dtypes.bfloat16) for f in (np.cos, np.sin)]
    return [table.astype(np.float32) for table in rounded]


def kernel_tables(width, length, n, samples, rows):
    local = MODES // n
    cosine, sine = host_tables(width, MODES)
    forward = np.stack([cosine.T, -sine.T], axis=1)
    doubled = forward * np.where(np.arange(MODES) == 0, 1.0, 2.0)[:, None, None]

    def spread(table):
        table = table.reshape(n, local, 2, width)
        whole = np.zeros((n, samples, local, 2, width, samples), np.float32)
        for s in range(samples):
            whole[:, s, :, :, :, s] = table
        return whole.reshape(n * samples * local * 2, width * samples)

    cosine, sine = host_tables(length, length)
    upper = np.stack([cosine, sine], axis=2)
    lower = np.stack([-sine, cosine], axis=2)
    turn = np.stack([upper, lower], axis=0)
    both = samples * local
    mixing = np.zeros((2, both, length, length, both, 2), np.float32)
    for x in range(both):
        mixing[:, x, :, :, x, :] = turn
    mixing = mixing.reshape(2 * both * length, length * both * 2)

    flat = [
        spread(forward),
        spread(doubled),
        spread(doubled).T,
        spread(forward).T,
        mixing,
    ]
    return [np.ascontiguousarray(t).astype(ml_dtypes.bfloat16) for t in flat]


def dot(a, b, contract=(1, 0)):
    return lax.dot_general(
        a, b, (((contract[0],), (contract[1],)), ((), ())), preferred_element_type=jnp.float32
    )


def mixer(
    n,
    inner,
    divisor,
    tok_far,
    cot_far,
    col_tok_far,
    col_cot_far,
    inv_mix_far,
    inv_grad_far,
    turn_far,
    in_weight_far,
    in_bias_far,
    out_weight_far,
    out_bias_far,
    mixed,
    grad,
    in_weight_grad,
    in_bias_grad,
    out_weight_grad,
    out_bias_grad,
    tok,
    cot,
    col_tok,
    col_cot,
    inv_mix,
    inv_grad,
    turn,
    in_weight,
    in_bias,
    out_weight,
    out_bias,
    send_a,
    send_b,
    send_c,
    send_d,
    recv_a,
    recv_b,
    recv_c,
    recv_d,
    send_e,
    send_f,
    recv_e,
    recv_f,
    turn_back,
    wide,
    spec,
    hid,
    slope,
    inc,
    pre,
    mixed_modes,
    grads,
    halves,
    half_in,
    gathered,
    other,
    both,
    send_sem,
    recv_sem,
    pair_send,
    pair_recv,
    load_sem,
):
    me = lax.axis_index("seq")
    core = lax.axis_index("rep")
    partner = 1 - core
    rows, width, samples, channels = tok.shape
    groups = channels // GROUP
    outer = n // inner
    across, within = me // inner, lax.rem(me, inner)
    chunk = send_a.shape[2]
    row_chunk = chunk // rows
    bf16 = jnp.bfloat16

    barrier = pltpu.get_barrier_semaphore()

    def greet(j, carry):
        peer = lax.rem(me + j, n)
        pl.semaphore_signal(barrier, inc=1, device_id={"seq": peer}, device_id_type=MESH_ID)
        return carry

    lax.fori_loop(1, n, greet, 0)
    pl.semaphore_signal(barrier, inc=1, device_id={"rep": partner}, device_id_type=MESH_ID)

    moves = [(col_tok_far, col_tok)]
    moves += [(tok_far.at[h], tok.at[h]) for h in range(rows)]
    moves += [(col_cot_far, col_cot)]
    moves += [(cot_far.at[h], cot.at[h]) for h in range(rows)]
    moves += [
        (in_weight_far, in_weight),
        (out_weight_far, out_weight),
        (turn_far, turn),
        (in_bias_far, in_bias),
        (out_bias_far, out_bias),
        (inv_mix_far, inv_mix),
        (inv_grad_far, inv_grad),
    ]
    loads = [
        pltpu.make_async_copy(far, near, load_sem.at[i]) for i, (far, near) in enumerate(moves)
    ]
    for load in loads[: rows + 1]:
        load.start()

    def copy_to(slot, peer, source, target):
        return pltpu.make_async_remote_copy(
            src_ref=source,
            dst_ref=target,
            send_sem=send_sem.at[slot],
            recv_sem=recv_sem.at[slot],
            device_id={"seq": peer},
            device_id_type=MESH_ID,
        )

    def loop(count, act):
        def step(j, carry):
            act(j)
            return carry

        lax.fori_loop(1, count, step, 0)

    def peer_at(j):
        peer = jnp.int32(0)
        bit = 1
        while bit < n:
            peer = peer + bit * lax.rem(me // bit + j // bit, 2)
            bit *= 2
        return peer

    class Move:
        def __init__(self, slot, count, to, source, target, span):
            self.slot, self.count, self.to = slot, count, to
            self.source, self.target, self.span = source, target, span

        def start(self):
            def out(j):
                at, peer = self.to(j)
                copy_to(self.slot, peer, self.source(at), self.target).start()

            loop(self.count, out)

        def all(self):
            return copy_to(self.slot, me, self.span, self.span)

        def arrived(self):
            self.all().wait_recv()

        def left(self):
            self.all().wait_send()

    def to_peer(j):
        peer = peer_at(j)
        return peer, peer

    def to_plane(j):
        v = lax.rem(within + j, inner)
        return v, across * inner + v

    def everyone(slot, source, target, g, at=None):
        cut = pl.ds(0, chunk) if at is None else at
        return Move(
            slot,
            n,
            to_peer,
            lambda peer: source.at[g, peer, cut],
            target.at[g, me, cut],
            target.at[g, pl.ds(0, n - 1), cut],
        )

    def move_a(g):
        return everyone(g, send_a, recv_a, g)

    def move_b(g):
        return everyone(groups + g, send_b, recv_b, g)

    def move_c(g, h):
        at = pl.ds(h * row_chunk, row_chunk)
        return everyone(2 * groups + g * rows + h, send_c, recv_c, g, at)

    def move_d(g, h):
        at = pl.ds(h * row_chunk, row_chunk)
        return everyone((2 + rows) * groups + g * rows + h, send_d, recv_d, g, at)

    tail = (2 + 2 * rows) * groups
    move_e = Move(
        tail,
        inner,
        to_plane,
        lambda v: send_e.at[v],
        recv_e.at[within],
        recv_e.at[pl.ds(0, inner - 1)],
    )
    move_f = copy_to(tail + 1, (1 - across) * inner + within, send_f, recv_f)
    move_g = Move(
        tail + 2,
        inner,
        to_plane,
        lambda v: gathered.at[within],
        gathered.at[within],
        gathered.at[pl.ds(0, inner - 1)],
    )

    def lanes(g):
        return pl.ds(pl.multiple_of(g * GROUP, GROUP), GROUP)

    def fixed(g):
        return pl.ds(g * GROUP, GROUP)

    def columns(tokens, table, send, g):
        for h in range(rows):
            section = tokens[h, :, :, fixed(g)].reshape(width * samples, GROUP)
            send[g, :, h * row_chunk : (h + 1) * row_chunk, :] = (
                dot(table[...], section).astype(bf16).reshape(n, row_chunk, GROUP)
            )

    for load in loads[: rows + 1]:
        load.wait()
    for load in loads[rows + 1 :]:
        load.start()
    for g in range(groups):
        columns(tok, col_tok, send_a, g)
        if g == 0:
            pl.semaphore_wait(barrier, n)
        move_a(g).start()
        if g == 0:
            for load in loads[rows + 1 : 2 * rows + 2]:
                load.wait()
        columns(cot, col_cot, send_b, g)
        move_b(g).start()
    for load in loads[2 * rows + 2 :]:
        load.wait()
    recv_a[:, me] = send_a[:, me]
    recv_b[:, me] = send_b[:, me]

    turn_back[...] = turn[...].T
    row_at = lax.broadcasted_iota(jnp.int32, (BLOCK, GROUP), 0)
    lane_at = lax.broadcasted_iota(jnp.int32, (BLOCK, GROUP), 1)
    for at, weight in enumerate((in_weight, out_weight)):
        for i in range(PER_GROUP):
            place = (lane_at == row_at + i * BLOCK).astype(bf16)
            for c in range(2):
                for g in range(groups):
                    wide[2 * at + c, g, i * BLOCK : (i + 1) * BLOCK, :] = dot(
                        weight[c, g * PER_GROUP + i], place
                    ).astype(bf16)

    half = turn.shape[0] // 2
    scale = math.sqrt(2.0 / math.pi)

    def per_group(act):
        def step(g, carry):
            act(g, lanes(g))
            return carry

        lax.fori_loop(0, groups, step, 0)

    def along_rows(recv, keep, g):
        keep[g] = dot(turn[...], recv[g].reshape(turn.shape[1], GROUP)).astype(bf16)

    def back_rows(send, g):
        send[g] = dot(turn_back[...], mixed_modes[...]).astype(bf16).reshape(n, chunk, GROUP)

    def forward_group(g, at):
        along_rows(recv_a, spec, g)
        re, im = spec[g, :half], spec[g, half:]
        w_re, w_im = wide[0, g], wide[1, g]
        for c in range(2):
            if c == 0:
                value = dot(re, w_re) - dot(im, w_im)
            else:
                value = dot(re, w_im) + dot(im, w_re)
            value = value + in_bias[c : c + 1, at]
            square = value * value
            tanh = jnp.tanh(scale * value * (1.0 + 0.044715 * square))
            hid[g, c * half : (c + 1) * half] = (0.5 * value * (1.0 + tanh)).astype(bf16)
            slope[g, c * half : (c + 1) * half] = 0.5 * (1.0 + tanh) + 0.5 * value * (
                1.0 - tanh * tanh
            ) * (scale * (1.0 + (3.0 * 0.044715) * square))
        re, im = hid[g, :half], hid[g, half:]
        w_re, w_im = wide[2, g], wide[3, g]
        mixed_modes[:half] = (
            dot(re, w_re) - dot(im, w_im) + out_bias[0:1, at]
        ).astype(bf16)
        mixed_modes[half:] = (
            dot(re, w_im) + dot(im, w_re) + out_bias[1:2, at]
        ).astype(bf16)
        back_rows(send_c, g)

    def backward_group(g):
        along_rows(recv_b, inc, g)
        re, im = inc[g, :half], inc[g, half:]
        w_re, w_im = wide[2, g], wide[3, g]
        pre[g, :half] = (
            (dot(re, w_re, (1, 1)) + dot(im, w_im, (1, 1))) * slope[g, :half]
        ).astype(bf16)
        pre[g, half:] = (
            (dot(im, w_re, (1, 1)) - dot(re, w_im, (1, 1))) * slope[g, half:]
        ).astype(bf16)
        re, im = pre[g, :half], pre[g, half:]
        w_re, w_im = wide[0, g], wide[1, g]
        mixed_modes[:half] = (dot(re, w_re, (1, 1)) + dot(im, w_im, (1, 1))).astype(bf16)
        mixed_modes[half:] = (dot(im, w_re, (1, 1)) - dot(re, w_im, (1, 1))).astype(bf16)
        back_rows(send_d, g)

    def fold(product):
        total = jnp.zeros((BLOCK, GROUP), jnp.float32)
        for i in range(PER_GROUP):
            inside = (lane_at >= i * BLOCK) & (lane_at < (i + 1) * BLOCK)
            total = jnp.where(inside, product[i * BLOCK : (i + 1) * BLOCK], total)
        return total.astype(bf16)

    bias_at = lax.broadcasted_iota(jnp.int32, (16, GROUP), 0)

    def grads_group(g, at):
        bias = jnp.zeros((16, GROUP), jnp.float32)
        for k, (left, right) in enumerate(((spec, pre), (hid, inc))):
            a_re, a_im = left[g, :half], left[g, half:]
            b_re, b_im = right[g, :half], right[g, half:]
            first = 2 * k * BLOCK
            grads[first : first + BLOCK, at] = fold(
                dot(a_re, b_re, (0, 0)) + dot(a_im, b_im, (0, 0))
            )
            grads[first + BLOCK : first + 2 * BLOCK, at] = fold(
                dot(a_re, b_im, (0, 0)) - dot(a_im, b_re, (0, 0))
            )
            for c, value in enumerate((b_re, b_im)):
                total = jnp.sum(value.astype(jnp.float32), axis=0, keepdims=True)
                bias = jnp.where(bias_at == 2 * k + c, total, bias)
        grads[4 * BLOCK : 4 * BLOCK + 16, at] = bias.astype(bf16)

    last = groups - 1
    held = [move_c(last, h) for h in range(rows)]
    held += [move_d(g, h) for g in range(groups) for h in range(rows)]

    def release(count):
        for move in held[:count]:
            move.start()
        del held[:count]

    def mix_group(g, at):
        with jax.named_scope("wait_a"):
            move_a(g).arrived()
        with jax.named_scope("fwd"):
            forward_group(g, at)
        recv_c[g, me] = send_c[g, me]

        @pl.when(g < last)
        def _():
            for h in range(rows):
                move_c(g, h).start()

        with jax.named_scope("wait_b"):
            move_b(g).arrived()

        @pl.when(g == last)
        def _():
            release(FIRST)

        with jax.named_scope("bwd"):
            backward_group(g)
        recv_d[g, me] = send_d[g, me]
        with jax.named_scope("grads"):
            grads_group(g, at)

    per_group(mix_group)

    per = 4 * BLOCK // (2 * n)
    to_row = lax.broadcasted_iota(jnp.int32, (2 * n * 16, 4 * BLOCK + 16), 0)
    from_row = lax.broadcasted_iota(jnp.int32, (2 * n * 16, 4 * BLOCK + 16), 1)
    slot = to_row % 16
    wanted = jnp.where(slot < per, to_row // 16 * per + slot, 4 * BLOCK + slot - per)
    picks = (wanted == from_row).astype(bf16)
    halves[...] = dot(picks, grads[...]).astype(bf16).reshape(halves.shape)

    def swap(slot, source, target):
        return pltpu.make_async_remote_copy(
            src_ref=source,
            dst_ref=target,
            send_sem=pair_send.at[slot],
            recv_sem=pair_recv.at[slot],
            device_id={"rep": partner},
            device_id_type=MESH_ID,
        )

    first_swap = swap(0, halves.at[partner], half_in)
    first_swap.start()

    def inverse_row(h, g, tokens, table, recv, out):
        section = recv[g, :, h * row_chunk : (h + 1) * row_chunk, :]
        product = dot(table[...], section.reshape(n * row_chunk, GROUP))
        kept = tokens[h, :, :, fixed(g)].reshape(width * samples, GROUP).astype(jnp.float32)
        out[h, :, :, fixed(g)] = (kept + product).astype(bf16).reshape(width, samples, GROUP)

    with jax.named_scope("swap1"):
        first_swap.wait()
    send_e[...] = (
        (halves[core].astype(jnp.float32) + half_in[...].astype(jnp.float32))
        .astype(bf16)
        .reshape(send_e.shape)
    )
    move_e.start()
    recv_e[within] = send_e[within]
    release(AFTER_E)
    with jax.named_scope("wait_e"):
        move_e.arrived()
    send_f[...] = jnp.sum(recv_e[...].astype(jnp.float32), axis=0).astype(bf16)
    move_f.start()
    release(AFTER_F)
    with jax.named_scope("wait_f"):
        move_f.wait_recv()
    total = (send_f[...].astype(jnp.float32) + recv_f[...].astype(jnp.float32)) * (1.0 / divisor)
    in_bias_grad[...] = total[0, per : per + 2]
    out_bias_grad[...] = total[0, per + 2 : per + 4]
    gathered[within] = total.astype(bf16)
    move_g.start()
    release(len(held))
    def finish_c(g, h):
        with jax.named_scope(f"wait_c{g}{h}"):
            move_c(g, h).arrived()
        inverse_row(h, g, tok, inv_mix, recv_c, mixed)

    def finish_d(g, h):
        with jax.named_scope(f"wait_d{g}{h}"):
            move_d(g, h).arrived()
        inverse_row(h, g, cot, inv_grad, recv_d, grad)

    for g in range(groups):
        for h in range(rows):
            finish_c(g, h)
    for g in range(groups):
        move_a(g).left()
        move_b(g).left()
    move_e.left()
    move_f.wait_send()
    for g in range(last):
        for h in range(rows):
            finish_d(g, h)
    with jax.named_scope("wait_g"):
        move_g.arrived()
    last_swap = swap(1, gathered, other)
    last_swap.start()
    both[core] = gathered[...].reshape(n * 16, channels)
    move_g.left()
    for g in range(groups):
        for h in range(rows):
            move_c(g, h).left()
    for h in range(rows - 1):
        finish_d(last, h)
    with jax.named_scope("swap2"):
        last_swap.wait()
    both[partner] = other[...].reshape(n * 16, channels)
    to_row = lax.broadcasted_iota(jnp.int32, (2 * BLOCK, n * 16), 0)
    from_row = lax.broadcasted_iota(jnp.int32, (2 * BLOCK, n * 16), 1)
    order = (to_row // per * 16 + to_row % per == from_row).astype(bf16)
    with jax.named_scope("params"):
        for k, out in enumerate((in_weight_grad, out_weight_grad)):
            for g in range(groups):
                ordered = dot(order, both[k, :, g * GROUP : (g + 1) * GROUP]).astype(bf16)
                for i in range(PER_GROUP):
                    place = (lane_at == row_at + i * BLOCK).astype(bf16)
                    block = dot(ordered, place, (1, 1))
                    for c in range(2):
                        out[c, g * PER_GROUP + i] = block[c * BLOCK : (c + 1) * BLOCK]
    finish_d(last, rows - 1)
    with jax.named_scope("end"):
        for g in range(groups):
            for h in range(rows):
                move_d(g, h).left()


def settle(*refs):
    count = len(refs) // 2
    near, far, sems = refs[:count], refs[count:-1], refs[-1]
    copies = [
        pltpu.make_async_copy(a, b, sems.at[i]) for i, (a, b) in enumerate(zip(near, far))
    ]
    for copy in copies:
        copy.start()
    for copy in copies:
        copy.wait()


def fits(n, reps, samples, rows, channels):
    per_row = samples * (MODES // n) * 2
    return (
        reps == 2
        and MODES % n == 0
        and per_row % 16 == 0
        and channels % GROUP == 0
        and channels == BLOCKS * BLOCK
        and (4 * BLOCK) % (2 * n) == 0
        and n > 3
        and n & (n - 1) == 0
        and rows > 1
        and 4 * BLOCK // (2 * n) + 4 <= 16
        and (samples * MODES // n * rows * n) % 16 == 0
    )


def shards(tokens, cotangent, in_weight, in_bias, out_weight, out_bias):
    samples, rows, width, channels = tokens.shape
    n, reps = lax.axis_size("seq"), lax.axis_size("rep")
    if not fits(n, reps, samples, rows, channels):
        return shards_plain(tokens, cotangent, in_weight, in_bias, out_weight, out_bias)
    length = rows * n
    outer = 2
    inner = n // outer
    chunk = rows * samples * (MODES // n) * 2
    whole = n * chunk
    groups = channels // GROUP
    tables = [jnp.asarray(t) for t in kernel_tables(width, length, n, samples, rows)]
    bf16, f32 = jnp.bfloat16, jnp.float32
    block = pltpu.VMEM((groups, n, chunk, GROUP), bf16)
    small = pltpu.VMEM((n, 16, channels), bf16)
    ringed = pltpu.VMEM((inner, outer, 16, channels), bf16)
    lined = pltpu.VMEM((outer, 16, channels), bf16)
    planes = (tokens.transpose(1, 2, 0, 3), cotangent.transpose(1, 2, 0, 3))
    kept = pltpu.VMEM((groups, whole, GROUP), bf16)
    anywhere = pl.BlockSpec(memory_space=pl.ANY)
    far = pl.BlockSpec(memory_space=pltpu.HBM)
    inputs = (*planes, *tables, in_weight, in_bias, out_weight, out_bias)
    shapes = (
        (planes[0].shape, bf16),
        (planes[1].shape, bf16),
        (in_weight.shape, f32),
        (in_bias.shape, f32),
        (out_weight.shape, f32),
        (out_bias.shape, f32),
    )
    near = pl.pallas_call(
        functools.partial(mixer, n, inner, float(samples * reps)),
        out_shape=tuple(pltpu.VMEM(*shape) for shape in shapes),
        in_specs=[far] * 11,
        grid=(1,),
        out_specs=(pl.BlockSpec(memory_space=pltpu.VMEM),) * 6,
        scratch_shapes=[pltpu.VMEM(v.shape, v.dtype) for v in inputs]
        + [block] * 8
        + [ringed, lined] * 2
        + [
            pltpu.VMEM((whole, whole), bf16),
            pltpu.VMEM((4, groups, GROUP, GROUP), bf16),
            kept,
            kept,
            pltpu.VMEM((groups, whole, GROUP), f32),
            kept,
            kept,
            pltpu.VMEM((whole, GROUP), bf16),
            pltpu.VMEM((4 * BLOCK + 16, channels), bf16),
            pltpu.VMEM((2, n, 16, channels), bf16),
            small,
            ringed,
            ringed,
            pltpu.VMEM((2, n * 16, channels), bf16),
            pltpu.SemaphoreType.DMA(((2 + 2 * rows) * groups + 3,)),
            pltpu.SemaphoreType.DMA(((2 + 2 * rows) * groups + 3,)),
            pltpu.SemaphoreType.DMA((2,)),
            pltpu.SemaphoreType.DMA((2,)),
            pltpu.SemaphoreType.DMA((2 * rows + 9,)),
        ],
        compiler_params=pltpu.CompilerParams(
            collective_id=0, has_side_effects=True, vmem_limit_bytes=VMEM_LIMIT
        ),
        name="mixer",
    )(*inputs)
    mixed, grad, *parameter_grads = pl.pallas_call(
        settle,
        out_shape=tuple(jax.ShapeDtypeStruct(*shape) for shape in shapes),
        in_specs=[anywhere] * 6,
        out_specs=(far,) * 6,
        scratch_shapes=[pltpu.SemaphoreType.DMA((6,))],
        compiler_params=pltpu.CompilerParams(vmem_limit_bytes=1 << 20),
        name="settle",
    )(*(pltpu.with_memory_space_constraint(part, pltpu.VMEM) for part in near))
    return (
        mixed.transpose(2, 0, 1, 3),
        grad.transpose(2, 0, 1, 3),
        *parameter_grads,
    )


def solution(mesh):
    in_specs = (P("rep", "seq", None, None), P("rep", "seq", None, None), P(), P(), P(), P())
    out_specs = (P("rep", "seq", None, None), P("rep", "seq", None, None), P(), P(), P(), P())
    return jax.shard_map(shards, mesh=mesh, in_specs=in_specs, out_specs=out_specs, check_vma=False)
```

```python
import functools
import math

import jax
import jax.numpy as jnp
import ml_dtypes
import numpy as np
from jax import lax
from jax.experimental import pallas as pl
from jax.experimental.pallas import tpu as pltpu
from jax.sharding import PartitionSpec as P

BLOCKS = 8
BLOCK = 96
MODES = 64


def grid_tables(length, modes):
    position = jnp.arange(length, dtype=jnp.int32)
    frequency = jnp.arange(modes, dtype=jnp.int32)
    residue = position[:, None] * frequency[None, :] % length
    angles = residue.astype(jnp.float32) * (2.0 * math.pi / length)
    factor = 1.0 / math.sqrt(length)
    cosine_table = (jnp.cos(angles) * factor).astype(jnp.bfloat16)
    sine_table = (jnp.sin(angles) * factor).astype(jnp.bfloat16)
    return (cosine_table, sine_table)


def column_tables(grid_width, modes):
    cosine_table, sine_table = grid_tables(grid_width, modes)
    forward = jnp.stack([cosine_table, -sine_table], axis=2)
    doubling = jnp.where(jnp.arange(modes) == 0, 1.0, 2.0).astype(jnp.bfloat16)[:, None]
    inverse = jnp.stack([cosine_table.T * doubling, -(sine_table.T * doubling)], axis=1)
    return (forward, inverse)


def row_table(length):
    cosine_table, sine_table = grid_tables(length, length)
    upper_rows = jnp.stack([cosine_table, sine_table], axis=2)
    lower_rows = jnp.stack([-sine_table, cosine_table], axis=2)
    return jnp.stack([upper_rows, lower_rows], axis=1)


def block_weights(weight):
    real_part, imag_part = (weight[0], weight[1])
    upper_half = jnp.stack([real_part, imag_part], axis=2)
    lower_half = jnp.stack([-imag_part, real_part], axis=2)
    return jnp.stack([upper_half, lower_half], axis=1)


def fold_blocks(blockwise):
    real_part = blockwise[:, 0, :, 0, :] + blockwise[:, 1, :, 1, :]
    imag_part = blockwise[:, 0, :, 1, :] - blockwise[:, 1, :, 0, :]
    return jnp.stack([real_part, imag_part])


def mix_forward(spectrum, weights_in, weights_out, bias_in, bias_out):
    mode_count = spectrum.shape[0] * spectrum.shape[1] * spectrum.shape[2]
    flat_modes = spectrum.reshape(mode_count, 2, BLOCKS, BLOCK)
    hidden_pre = (
        jnp.einsum("mcbi,bciej->mebj", flat_modes, weights_in, preferred_element_type=jnp.float32)
        + bias_in
    )
    hidden = jax.nn.gelu(hidden_pre).astype(jnp.bfloat16)
    spectrum_out = (
        jnp.einsum("mcbi,bciej->mebj", hidden, weights_out, preferred_element_type=jnp.float32)
        + bias_out
    )
    return (
        flat_modes,
        hidden_pre,
        hidden,
        spectrum_out.astype(jnp.bfloat16).reshape(spectrum.shape),
    )


def mix_backward(flat_modes, hidden_pre, hidden, incoming, weights_in, weights_out):
    incoming_flat = incoming.reshape(flat_modes.shape)
    out_bias_part = jnp.sum(incoming_flat.astype(jnp.float32), axis=0).reshape(2, -1)
    out_weight_part = fold_blocks(
        jnp.einsum("mcbi,mebj->bciej", hidden, incoming_flat, preferred_element_type=jnp.float32)
    )
    hidden_grad = jnp.einsum(
        "mebj,bciej->mcbi", incoming_flat, weights_out, preferred_element_type=jnp.float32
    )
    pre_grad = jax.vjp(jax.nn.gelu, hidden_pre)[1](hidden_grad)[0].astype(jnp.bfloat16)
    in_bias_part = jnp.sum(pre_grad.astype(jnp.float32), axis=0).reshape(2, -1)
    in_weight_part = fold_blocks(
        jnp.einsum("mcbi,mebj->bciej", flat_modes, pre_grad, preferred_element_type=jnp.float32)
    )
    spectrum_grad = jnp.einsum(
        "mebj,bciej->mcbi", pre_grad, weights_in, preferred_element_type=jnp.float32
    )
    spectrum_grad = spectrum_grad.astype(jnp.bfloat16).reshape(incoming.shape)
    return (spectrum_grad, (in_weight_part, in_bias_part, out_weight_part, out_bias_part))


def shards_plain(tokens, cotangent, in_weight, in_bias, out_weight, out_bias):
    samples, row_count, grid_width, channels = tokens.shape
    length = row_count * lax.axis_size("seq")
    column_forward, column_inverse = column_tables(grid_width, MODES)
    row_matrix = row_table(length)
    weights_in = block_weights(in_weight)
    weights_out = block_weights(out_weight)
    bias_in = in_bias.reshape(2, BLOCKS, BLOCK)
    bias_out = out_bias.reshape(2, BLOCKS, BLOCK)

    def along_rows(section):
        return jnp.einsum(
            "qehc,shkcd->sqked", row_matrix, section, preferred_element_type=jnp.float32
        ).astype(jnp.bfloat16)

    def back_rows(section):
        return jnp.einsum(
            "qehc,sqked->shkcd", row_matrix, section, preferred_element_type=jnp.float32
        ).astype(jnp.bfloat16)

    spec_rows = jnp.einsum(
        "shwd,wkc->shkcd", tokens, column_forward, preferred_element_type=jnp.float32
    ).astype(jnp.bfloat16)
    spectrum = along_rows(lax.all_to_all(spec_rows, "seq", split_axis=2, concat_axis=1, tiled=True))
    flat_modes, hidden_pre, hidden, spectrum_out = mix_forward(
        spectrum, weights_in, weights_out, bias_in, bias_out
    )
    mixed_grid = jnp.einsum(
        "shkcd,kcw->shwd",
        lax.all_to_all(back_rows(spectrum_out), "seq", split_axis=1, concat_axis=2, tiled=True),
        column_inverse,
        preferred_element_type=jnp.float32,
    )
    cot_rows = jnp.einsum(
        "shwd,kcw->shkcd", cotangent, column_inverse, preferred_element_type=jnp.float32
    ).astype(jnp.bfloat16)
    incoming = along_rows(lax.all_to_all(cot_rows, "seq", split_axis=2, concat_axis=1, tiled=True))
    spectrum_grad, partials = mix_backward(
        flat_modes, hidden_pre, hidden, incoming, weights_in, weights_out
    )
    adjoint_part = jnp.einsum(
        "shkcd,wkc->shwd",
        lax.all_to_all(back_rows(spectrum_grad), "seq", split_axis=1, concat_axis=2, tiled=True),
        column_forward,
        preferred_element_type=jnp.float32,
    )
    mixed_out = (tokens.astype(jnp.float32) + mixed_grid).astype(jnp.bfloat16)
    tokens_grad = (cotangent.astype(jnp.float32) + adjoint_part).astype(jnp.bfloat16)
    totals = lax.psum((partials[0], partials[1], partials[2], partials[3]), ("seq", "rep"))
    divisor = float(samples * lax.axis_size("rep"))
    return (
        mixed_out,
        tokens_grad,
        totals[0] / divisor,
        totals[1] / divisor,
        totals[2] / divisor,
        totals[3] / divisor,
    )


GROUP = math.lcm(BLOCK, 128)
PER_GROUP = GROUP // BLOCK
MESH_ID = pl.DeviceIdType.MESH
VMEM_LIMIT = 52 << 20
FIRST, AFTER_E, AFTER_F = 2, 3, 2
SPREAD = 11


def host_tables(length, modes):
    residue = np.arange(length)[:, None] * np.arange(modes)[None, :] % length
    angles = residue.astype(np.float32) * np.float32(2.0 * math.pi / length)
    factor = np.float32(1.0 / math.sqrt(length))
    rounded = [(f(angles) * factor).astype(ml_dtypes.bfloat16) for f in (np.cos, np.sin)]
    return [table.astype(np.float32) for table in rounded]


def kernel_tables(width, length, n, samples, rows):
    local = MODES // n
    cosine, sine = host_tables(width, MODES)
    forward = np.stack([cosine.T, -sine.T], axis=1)
    doubled = forward * np.where(np.arange(MODES) == 0, 1.0, 2.0)[:, None, None]

    def spread(table):
        table = table.reshape(n, local, 2, width)
        whole = np.zeros((n, samples, local, 2, width, samples), np.float32)
        for s in range(samples):
            whole[:, s, :, :, :, s] = table
        return whole.reshape(n * samples * local * 2, width * samples)

    cosine, sine = host_tables(length, length)
    upper = np.stack([cosine, sine], axis=2)
    lower = np.stack([-sine, cosine], axis=2)
    turn = np.stack([upper, lower], axis=0)
    both = samples * local
    mixing = np.zeros((2, both, length, length, both, 2), np.float32)
    for x in range(both):
        mixing[:, x, :, :, x, :] = turn
    mixing = mixing.reshape(2 * both * length, length * both * 2)

    flat = [
        spread(forward),
        spread(doubled),
        spread(doubled).T,
        spread(forward).T,
        mixing,
    ]
    return [np.ascontiguousarray(t).astype(ml_dtypes.bfloat16) for t in flat]


def dot(a, b, contract=(1, 0)):
    return lax.dot_general(
        a, b, (((contract[0],), (contract[1],)), ((), ())), preferred_element_type=jnp.float32
    )


def mixer(
    n,
    inner,
    divisor,
    tok_far,
    cot_far,
    col_tok_far,
    col_cot_far,
    inv_mix_far,
    inv_grad_far,
    turn_far,
    in_weight_far,
    in_bias_far,
    out_weight_far,
    out_bias_far,
    mixed,
    grad,
    in_weight_grad,
    in_bias_grad,
    out_weight_grad,
    out_bias_grad,
    tok,
    cot,
    col_tok,
    col_cot,
    inv_mix,
    inv_grad,
    turn,
    in_weight,
    in_bias,
    out_weight,
    out_bias,
    send_a,
    send_b,
    send_c,
    send_d,
    recv_a,
    recv_b,
    recv_c,
    recv_d,
    send_e,
    send_f,
    recv_e,
    recv_f,
    turn_back,
    wide,
    spec,
    hid,
    slope,
    inc,
    pre,
    mixed_modes,
    grads,
    halves,
    half_in,
    gathered,
    other,
    both,
    send_sem,
    recv_sem,
    pair_send,
    pair_recv,
    load_sem,
):
    me = lax.axis_index("seq")
    core = lax.axis_index("rep")
    partner = 1 - core
    rows, width, samples, channels = tok.shape
    groups = channels // GROUP
    outer = n // inner
    across, within = me // inner, lax.rem(me, inner)
    chunk = send_a.shape[2]
    row_chunk = chunk // rows
    bf16 = jnp.bfloat16

    barrier = pltpu.get_barrier_semaphore()

    def greet(j, carry):
        peer = lax.rem(me + j, n)
        pl.semaphore_signal(barrier, inc=1, device_id={"seq": peer}, device_id_type=MESH_ID)
        return carry

    lax.fori_loop(1, n, greet, 0)
    pl.semaphore_signal(barrier, inc=1, device_id={"rep": partner}, device_id_type=MESH_ID)

    moves = [(col_tok_far, col_tok)]
    moves += [(tok_far.at[h], tok.at[h]) for h in range(rows)]
    moves += [(col_cot_far, col_cot)]
    moves += [(cot_far.at[h], cot.at[h]) for h in range(rows)]
    moves += [
        (in_weight_far, in_weight),
        (out_weight_far, out_weight),
        (turn_far, turn),
        (in_bias_far, in_bias),
        (out_bias_far, out_bias),
        (inv_mix_far, inv_mix),
        (inv_grad_far, inv_grad),
    ]
    loads = [
        pltpu.make_async_copy(far, near, load_sem.at[i]) for i, (far, near) in enumerate(moves)
    ]
    for load in loads[: rows + 1]:
        load.start()

    def copy_to(slot, peer, source, target):
        return pltpu.make_async_remote_copy(
            src_ref=source,
            dst_ref=target,
            send_sem=send_sem.at[slot],
            recv_sem=recv_sem.at[slot],
            device_id={"seq": peer},
            device_id_type=MESH_ID,
        )

    def loop(count, act):
        def step(j, carry):
            act(j)
            return carry

        lax.fori_loop(1, count, step, 0)

    def peer_at(j):
        peer = jnp.int32(0)
        j = lax.rem(j * SPREAD, n)
        bit = 1
        while bit < n:
            peer = peer + bit * lax.rem(me // bit + j // bit, 2)
            bit *= 2
        return peer

    class Move:
        def __init__(self, slot, count, to, source, target, span):
            self.slot, self.count, self.to = slot, count, to
            self.source, self.target, self.span = source, target, span

        def start(self):
            def out(j):
                at, peer = self.to(j)
                copy_to(self.slot, peer, self.source(at), self.target).start()

            loop(self.count, out)

        def all(self):
            return copy_to(self.slot, me, self.span, self.span)

        def arrived(self):
            self.all().wait_recv()

        def left(self):
            self.all().wait_send()

    def to_peer(j):
        peer = peer_at(j)
        return peer, peer

    def to_plane(j):
        v = lax.rem(within + j, inner)
        return v, across * inner + v

    def everyone(slot, source, target, g, at=None):
        cut = pl.ds(0, chunk) if at is None else at
        return Move(
            slot,
            n,
            to_peer,
            lambda peer: source.at[g, peer, cut],
            target.at[g, me, cut],
            target.at[g, pl.ds(0, n - 1), cut],
        )

    def move_a(g):
        return everyone(g, send_a, recv_a, g)

    def move_b(g):
        return everyone(groups + g, send_b, recv_b, g)

    def move_c(g, h):
        at = pl.ds(h * row_chunk, row_chunk)
        return everyone(2 * groups + g * rows + h, send_c, recv_c, g, at)

    def move_d(g, h):
        at = pl.ds(h * row_chunk, row_chunk)
        return everyone((2 + rows) * groups + g * rows + h, send_d, recv_d, g, at)

    tail = (2 + 2 * rows) * groups
    move_e = Move(
        tail,
        inner,
        to_plane,
        lambda v: send_e.at[v],
        recv_e.at[within],
        recv_e.at[pl.ds(0, inner - 1)],
    )
    move_f = copy_to(tail + 1, (1 - across) * inner + within, send_f, recv_f)
    move_g = Move(
        tail + 2,
        inner,
        to_plane,
        lambda v: gathered.at[within],
        gathered.at[within],
        gathered.at[pl.ds(0, inner - 1)],
    )

    def lanes(g):
        return pl.ds(pl.multiple_of(g * GROUP, GROUP), GROUP)

    def fixed(g):
        return pl.ds(g * GROUP, GROUP)

    def columns(tokens, table, send, g):
        for h in range(rows):
            section = tokens[h, :, :, fixed(g)].reshape(width * samples, GROUP)
            send[g, :, h * row_chunk : (h + 1) * row_chunk, :] = (
                dot(table[...], section).astype(bf16).reshape(n, row_chunk, GROUP)
            )

    for load in loads[: rows + 1]:
        load.wait()
    for load in loads[rows + 1 :]:
        load.start()
    for g in range(groups):
        columns(tok, col_tok, send_a, g)
        if g == 0:
            pl.semaphore_wait(barrier, n)
        move_a(g).start()
        if g == 0:
            for load in loads[rows + 1 : 2 * rows + 2]:
                load.wait()
        columns(cot, col_cot, send_b, g)
        move_b(g).start()
    for load in loads[2 * rows + 2 :]:
        load.wait()
    recv_a[:, me] = send_a[:, me]
    recv_b[:, me] = send_b[:, me]

    turn_back[...] = turn[...].T
    row_at = lax.broadcasted_iota(jnp.int32, (BLOCK, GROUP), 0)
    lane_at = lax.broadcasted_iota(jnp.int32, (BLOCK, GROUP), 1)
    for at, weight in enumerate((in_weight, out_weight)):
        for i in range(PER_GROUP):
            place = (lane_at == row_at + i * BLOCK).astype(bf16)
            for c in range(2):
                for g in range(groups):
                    wide[2 * at + c, g, i * BLOCK : (i + 1) * BLOCK, :] = dot(
                        weight[c, g * PER_GROUP + i], place
                    ).astype(bf16)

    half = turn.shape[0] // 2
    scale = math.sqrt(2.0 / math.pi)

    def per_group(act):
        def step(g, carry):
            act(g, lanes(g))
            return carry

        lax.fori_loop(0, groups, step, 0)

    def along_rows(recv, keep, g):
        keep[g] = dot(turn[...], recv[g].reshape(turn.shape[1], GROUP)).astype(bf16)

    def back_rows(send, g):
        send[g] = dot(turn_back[...], mixed_modes[...]).astype(bf16).reshape(n, chunk, GROUP)

    def forward_group(g, at):
        along_rows(recv_a, spec, g)
        re, im = spec[g, :half], spec[g, half:]
        w_re, w_im = wide[0, g], wide[1, g]
        for c in range(2):
            if c == 0:
                value = dot(re, w_re) - dot(im, w_im)
            else:
                value = dot(re, w_im) + dot(im, w_re)
            value = value + in_bias[c : c + 1, at]
            square = value * value
            tanh = jnp.tanh(scale * value * (1.0 + 0.044715 * square))
            hid[g, c * half : (c + 1) * half] = (0.5 * value * (1.0 + tanh)).astype(bf16)
            slope[g, c * half : (c + 1) * half] = 0.5 * (1.0 + tanh) + 0.5 * value * (
                1.0 - tanh * tanh
            ) * (scale * (1.0 + (3.0 * 0.044715) * square))
        re, im = hid[g, :half], hid[g, half:]
        w_re, w_im = wide[2, g], wide[3, g]
        mixed_modes[:half] = (
            dot(re, w_re) - dot(im, w_im) + out_bias[0:1, at]
        ).astype(bf16)
        mixed_modes[half:] = (
            dot(re, w_im) + dot(im, w_re) + out_bias[1:2, at]
        ).astype(bf16)
        back_rows(send_c, g)

    def backward_group(g):
        along_rows(recv_b, inc, g)
        re, im = inc[g, :half], inc[g, half:]
        w_re, w_im = wide[2, g], wide[3, g]
        pre[g, :half] = (
            (dot(re, w_re, (1, 1)) + dot(im, w_im, (1, 1))) * slope[g, :half]
        ).astype(bf16)
        pre[g, half:] = (
            (dot(im, w_re, (1, 1)) - dot(re, w_im, (1, 1))) * slope[g, half:]
        ).astype(bf16)
        re, im = pre[g, :half], pre[g, half:]
        w_re, w_im = wide[0, g], wide[1, g]
        mixed_modes[:half] = (dot(re, w_re, (1, 1)) + dot(im, w_im, (1, 1))).astype(bf16)
        mixed_modes[half:] = (dot(im, w_re, (1, 1)) - dot(re, w_im, (1, 1))).astype(bf16)
        back_rows(send_d, g)

    def fold(product):
        total = jnp.zeros((BLOCK, GROUP), jnp.float32)
        for i in range(PER_GROUP):
            inside = (lane_at >= i * BLOCK) & (lane_at < (i + 1) * BLOCK)
            total = jnp.where(inside, product[i * BLOCK : (i + 1) * BLOCK], total)
        return total.astype(bf16)

    bias_at = lax.broadcasted_iota(jnp.int32, (16, GROUP), 0)

    def grads_group(g, at):
        bias = jnp.zeros((16, GROUP), jnp.float32)
        for k, (left, right) in enumerate(((spec, pre), (hid, inc))):
            a_re, a_im = left[g, :half], left[g, half:]
            b_re, b_im = right[g, :half], right[g, half:]
            first = 2 * k * BLOCK
            grads[first : first + BLOCK, at] = fold(
                dot(a_re, b_re, (0, 0)) + dot(a_im, b_im, (0, 0))
            )
            grads[first + BLOCK : first + 2 * BLOCK, at] = fold(
                dot(a_re, b_im, (0, 0)) - dot(a_im, b_re, (0, 0))
            )
            for c, value in enumerate((b_re, b_im)):
                total = jnp.sum(value.astype(jnp.float32), axis=0, keepdims=True)
                bias = jnp.where(bias_at == 2 * k + c, total, bias)
        grads[4 * BLOCK : 4 * BLOCK + 16, at] = bias.astype(bf16)

    last = groups - 1
    held = [move_c(last, h) for h in range(rows)]
    held += [move_d(g, h) for g in range(groups) for h in range(rows)]

    def release(count):
        for move in held[:count]:
            move.start()
        del held[:count]

    def mix_group(g, at):
        with jax.named_scope("wait_a"):
            move_a(g).arrived()
        with jax.named_scope("fwd"):
            forward_group(g, at)
        recv_c[g, me] = send_c[g, me]

        @pl.when(g < last)
        def _():
            for h in range(rows):
                move_c(g, h).start()

        with jax.named_scope("wait_b"):
            move_b(g).arrived()

        @pl.when(g == last)
        def _():
            release(FIRST)

        with jax.named_scope("bwd"):
            backward_group(g)
        recv_d[g, me] = send_d[g, me]
        with jax.named_scope("grads"):
            grads_group(g, at)

    per_group(mix_group)

    per = 4 * BLOCK // (2 * n)
    to_row = lax.broadcasted_iota(jnp.int32, (2 * n * 16, 4 * BLOCK + 16), 0)
    from_row = lax.broadcasted_iota(jnp.int32, (2 * n * 16, 4 * BLOCK + 16), 1)
    slot = to_row % 16
    wanted = jnp.where(slot < per, to_row // 16 * per + slot, 4 * BLOCK + slot - per)
    picks = (wanted == from_row).astype(bf16)
    halves[...] = dot(picks, grads[...]).astype(bf16).reshape(halves.shape)

    def swap(slot, source, target):
        return pltpu.make_async_remote_copy(
            src_ref=source,
            dst_ref=target,
            send_sem=pair_send.at[slot],
            recv_sem=pair_recv.at[slot],
            device_id={"rep": partner},
            device_id_type=MESH_ID,
        )

    first_swap = swap(0, halves.at[partner], half_in)
    first_swap.start()

    def inverse_row(h, g, tokens, table, recv, out):
        section = recv[g, :, h * row_chunk : (h + 1) * row_chunk, :]
        product = dot(table[...], section.reshape(n * row_chunk, GROUP))
        kept = tokens[h, :, :, fixed(g)].reshape(width * samples, GROUP).astype(jnp.float32)
        out[h, :, :, fixed(g)] = (kept + product).astype(bf16).reshape(width, samples, GROUP)

    with jax.named_scope("swap1"):
        first_swap.wait()
    send_e[...] = (
        (halves[core].astype(jnp.float32) + half_in[...].astype(jnp.float32))
        .astype(bf16)
        .reshape(send_e.shape)
    )
    move_e.start()
    recv_e[within] = send_e[within]
    release(AFTER_E)
    with jax.named_scope("wait_e"):
        move_e.arrived()
    send_f[...] = jnp.sum(recv_e[...].astype(jnp.float32), axis=0).astype(bf16)
    move_f.start()
    release(AFTER_F)
    with jax.named_scope("wait_f"):
        move_f.wait_recv()
    total = (send_f[...].astype(jnp.float32) + recv_f[...].astype(jnp.float32)) * (1.0 / divisor)
    in_bias_grad[...] = total[0, per : per + 2]
    out_bias_grad[...] = total[0, per + 2 : per + 4]
    gathered[within] = total.astype(bf16)
    move_g.start()
    release(len(held))
    def finish_c(g, h):
        with jax.named_scope(f"wait_c{g}{h}"):
            move_c(g, h).arrived()
        inverse_row(h, g, tok, inv_mix, recv_c, mixed)

    def finish_d(g, h):
        with jax.named_scope(f"wait_d{g}{h}"):
            move_d(g, h).arrived()
        inverse_row(h, g, cot, inv_grad, recv_d, grad)

    for g in range(groups):
        for h in range(rows):
            finish_c(g, h)
    for g in range(groups):
        move_a(g).left()
        move_b(g).left()
    move_e.left()
    move_f.wait_send()
    for g in range(last):
        for h in range(rows):
            finish_d(g, h)
    with jax.named_scope("wait_g"):
        move_g.arrived()
    last_swap = swap(1, gathered, other)
    last_swap.start()
    both[core] = gathered[...].reshape(n * 16, channels)
    move_g.left()
    for g in range(groups):
        for h in range(rows):
            move_c(g, h).left()
    finish_d(last, 0)
    with jax.named_scope("swap2"):
        last_swap.wait()
    both[partner] = other[...].reshape(n * 16, channels)
    to_row = lax.broadcasted_iota(jnp.int32, (2 * BLOCK, n * 16), 0)
    from_row = lax.broadcasted_iota(jnp.int32, (2 * BLOCK, n * 16), 1)
    order = (to_row // per * 16 + to_row % per == from_row).astype(bf16)
    with jax.named_scope("params"):
        for k, out in enumerate((in_weight_grad, out_weight_grad)):
            for g in range(groups):
                ordered = dot(order, both[k, :, g * GROUP : (g + 1) * GROUP]).astype(bf16)
                for i in range(PER_GROUP):
                    place = (lane_at == row_at + i * BLOCK).astype(bf16)
                    block = dot(ordered, place, (1, 1))
                    for c in range(2):
                        out[c, g * PER_GROUP + i] = block[c * BLOCK : (c + 1) * BLOCK]
    for h in range(1, rows):
        finish_d(last, h)
    with jax.named_scope("end"):
        for g in range(groups):
            for h in range(rows):
                move_d(g, h).left()


def settle(*refs):
    count = len(refs) // 2
    near, far, sems = refs[:count], refs[count:-1], refs[-1]
    copies = [
        pltpu.make_async_copy(a, b, sems.at[i]) for i, (a, b) in enumerate(zip(near, far))
    ]
    for copy in copies:
        copy.start()
    for copy in copies:
        copy.wait()


def fits(n, reps, samples, rows, channels):
    per_row = samples * (MODES // n) * 2
    return (
        reps == 2
        and MODES % n == 0
        and per_row % 16 == 0
        and channels % GROUP == 0
        and channels == BLOCKS * BLOCK
        and (4 * BLOCK) % (2 * n) == 0
        and n > 3
        and n & (n - 1) == 0
        and rows > 1
        and 4 * BLOCK // (2 * n) + 4 <= 16
        and (samples * MODES // n * rows * n) % 16 == 0
    )


def shards(tokens, cotangent, in_weight, in_bias, out_weight, out_bias):
    samples, rows, width, channels = tokens.shape
    n, reps = lax.axis_size("seq"), lax.axis_size("rep")
    if not fits(n, reps, samples, rows, channels):
        return shards_plain(tokens, cotangent, in_weight, in_bias, out_weight, out_bias)
    length = rows * n
    outer = 2
    inner = n // outer
    chunk = rows * samples * (MODES // n) * 2
    whole = n * chunk
    groups = channels // GROUP
    tables = [jnp.asarray(t) for t in kernel_tables(width, length, n, samples, rows)]
    bf16, f32 = jnp.bfloat16, jnp.float32
    block = pltpu.VMEM((groups, n, chunk, GROUP), bf16)
    small = pltpu.VMEM((n, 16, channels), bf16)
    ringed = pltpu.VMEM((inner, outer, 16, channels), bf16)
    lined = pltpu.VMEM((outer, 16, channels), bf16)
    planes = (tokens.transpose(1, 2, 0, 3), cotangent.transpose(1, 2, 0, 3))
    kept = pltpu.VMEM((groups, whole, GROUP), bf16)
    anywhere = pl.BlockSpec(memory_space=pl.ANY)
    far = pl.BlockSpec(memory_space=pltpu.HBM)
    inputs = (*planes, *tables, in_weight, in_bias, out_weight, out_bias)
    shapes = (
        (planes[0].shape, bf16),
        (planes[1].shape, bf16),
        (in_weight.shape, f32),
        (in_bias.shape, f32),
        (out_weight.shape, f32),
        (out_bias.shape, f32),
    )
    near = pl.pallas_call(
        functools.partial(mixer, n, inner, float(samples * reps)),
        out_shape=tuple(pltpu.VMEM(*shape) for shape in shapes),
        in_specs=[far] * 11,
        grid=(1,),
        out_specs=(pl.BlockSpec(memory_space=pltpu.VMEM),) * 6,
        scratch_shapes=[pltpu.VMEM(v.shape, v.dtype) for v in inputs]
        + [block] * 8
        + [ringed, lined] * 2
        + [
            pltpu.VMEM((whole, whole), bf16),
            pltpu.VMEM((4, groups, GROUP, GROUP), bf16),
            kept,
            kept,
            pltpu.VMEM((groups, whole, GROUP), f32),
            kept,
            kept,
            pltpu.VMEM((whole, GROUP), bf16),
            pltpu.VMEM((4 * BLOCK + 16, channels), bf16),
            pltpu.VMEM((2, n, 16, channels), bf16),
            small,
            ringed,
            ringed,
            pltpu.VMEM((2, n * 16, channels), bf16),
            pltpu.SemaphoreType.DMA(((2 + 2 * rows) * groups + 3,)),
            pltpu.SemaphoreType.DMA(((2 + 2 * rows) * groups + 3,)),
            pltpu.SemaphoreType.DMA((2,)),
            pltpu.SemaphoreType.DMA((2,)),
            pltpu.SemaphoreType.DMA((2 * rows + 9,)),
        ],
        compiler_params=pltpu.CompilerParams(
            collective_id=0, has_side_effects=True, vmem_limit_bytes=VMEM_LIMIT
        ),
        name="mixer",
    )(*inputs)
    mixed, grad, *parameter_grads = pl.pallas_call(
        settle,
        out_shape=tuple(jax.ShapeDtypeStruct(*shape) for shape in shapes),
        in_specs=[anywhere] * 6,
        out_specs=(far,) * 6,
        scratch_shapes=[pltpu.SemaphoreType.DMA((6,))],
        compiler_params=pltpu.CompilerParams(vmem_limit_bytes=1 << 20),
        name="settle",
    )(*(pltpu.with_memory_space_constraint(part, pltpu.VMEM) for part in near))
    return (
        mixed.transpose(2, 0, 1, 3),
        grad.transpose(2, 0, 1, 3),
        *parameter_grads,
    )


def solution(mesh):
    in_specs = (P("rep", "seq", None, None), P("rep", "seq", None, None), P(), P(), P(), P())
    out_specs = (P("rep", "seq", None, None), P("rep", "seq", None, None), P(), P(), P(), P())
    return jax.shard_map(shards, mesh=mesh, in_specs=in_specs, out_specs=out_specs, check_vma=False)
```

```python
import functools
import math

import jax
import jax.numpy as jnp
import ml_dtypes
import numpy as np
from jax import lax
from jax.experimental import pallas as pl
from jax.experimental.pallas import tpu as pltpu
from jax.sharding import PartitionSpec as P

BLOCKS = 8
BLOCK = 96
MODES = 64


def grid_tables(length, modes):
    position = jnp.arange(length, dtype=jnp.int32)
    frequency = jnp.arange(modes, dtype=jnp.int32)
    residue = position[:, None] * frequency[None, :] % length
    angles = residue.astype(jnp.float32) * (2.0 * math.pi / length)
    factor = 1.0 / math.sqrt(length)
    cosine_table = (jnp.cos(angles) * factor).astype(jnp.bfloat16)
    sine_table = (jnp.sin(angles) * factor).astype(jnp.bfloat16)
    return (cosine_table, sine_table)


def column_tables(grid_width, modes):
    cosine_table, sine_table = grid_tables(grid_width, modes)
    forward = jnp.stack([cosine_table, -sine_table], axis=2)
    doubling = jnp.where(jnp.arange(modes) == 0, 1.0, 2.0).astype(jnp.bfloat16)[:, None]
    inverse = jnp.stack([cosine_table.T * doubling, -(sine_table.T * doubling)], axis=1)
    return (forward, inverse)


def row_table(length):
    cosine_table, sine_table = grid_tables(length, length)
    upper_rows = jnp.stack([cosine_table, sine_table], axis=2)
    lower_rows = jnp.stack([-sine_table, cosine_table], axis=2)
    return jnp.stack([upper_rows, lower_rows], axis=1)


def block_weights(weight):
    real_part, imag_part = (weight[0], weight[1])
    upper_half = jnp.stack([real_part, imag_part], axis=2)
    lower_half = jnp.stack([-imag_part, real_part], axis=2)
    return jnp.stack([upper_half, lower_half], axis=1)


def fold_blocks(blockwise):
    real_part = blockwise[:, 0, :, 0, :] + blockwise[:, 1, :, 1, :]
    imag_part = blockwise[:, 0, :, 1, :] - blockwise[:, 1, :, 0, :]
    return jnp.stack([real_part, imag_part])


def mix_forward(spectrum, weights_in, weights_out, bias_in, bias_out):
    mode_count = spectrum.shape[0] * spectrum.shape[1] * spectrum.shape[2]
    flat_modes = spectrum.reshape(mode_count, 2, BLOCKS, BLOCK)
    hidden_pre = (
        jnp.einsum("mcbi,bciej->mebj", flat_modes, weights_in, preferred_element_type=jnp.float32)
        + bias_in
    )
    hidden = jax.nn.gelu(hidden_pre).astype(jnp.bfloat16)
    spectrum_out = (
        jnp.einsum("mcbi,bciej->mebj", hidden, weights_out, preferred_element_type=jnp.float32)
        + bias_out
    )
    return (
        flat_modes,
        hidden_pre,
        hidden,
        spectrum_out.astype(jnp.bfloat16).reshape(spectrum.shape),
    )


def mix_backward(flat_modes, hidden_pre, hidden, incoming, weights_in, weights_out):
    incoming_flat = incoming.reshape(flat_modes.shape)
    out_bias_part = jnp.sum(incoming_flat.astype(jnp.float32), axis=0).reshape(2, -1)
    out_weight_part = fold_blocks(
        jnp.einsum("mcbi,mebj->bciej", hidden, incoming_flat, preferred_element_type=jnp.float32)
    )
    hidden_grad = jnp.einsum(
        "mebj,bciej->mcbi", incoming_flat, weights_out, preferred_element_type=jnp.float32
    )
    pre_grad = jax.vjp(jax.nn.gelu, hidden_pre)[1](hidden_grad)[0].astype(jnp.bfloat16)
    in_bias_part = jnp.sum(pre_grad.astype(jnp.float32), axis=0).reshape(2, -1)
    in_weight_part = fold_blocks(
        jnp.einsum("mcbi,mebj->bciej", flat_modes, pre_grad, preferred_element_type=jnp.float32)
    )
    spectrum_grad = jnp.einsum(
        "mebj,bciej->mcbi", pre_grad, weights_in, preferred_element_type=jnp.float32
    )
    spectrum_grad = spectrum_grad.astype(jnp.bfloat16).reshape(incoming.shape)
    return (spectrum_grad, (in_weight_part, in_bias_part, out_weight_part, out_bias_part))


def shards_plain(tokens, cotangent, in_weight, in_bias, out_weight, out_bias):
    samples, row_count, grid_width, channels = tokens.shape
    length = row_count * lax.axis_size("seq")
    column_forward, column_inverse = column_tables(grid_width, MODES)
    row_matrix = row_table(length)
    weights_in = block_weights(in_weight)
    weights_out = block_weights(out_weight)
    bias_in = in_bias.reshape(2, BLOCKS, BLOCK)
    bias_out = out_bias.reshape(2, BLOCKS, BLOCK)

    def along_rows(section):
        return jnp.einsum(
            "qehc,shkcd->sqked", row_matrix, section, preferred_element_type=jnp.float32
        ).astype(jnp.bfloat16)

    def back_rows(section):
        return jnp.einsum(
            "qehc,sqked->shkcd", row_matrix, section, preferred_element_type=jnp.float32
        ).astype(jnp.bfloat16)

    spec_rows = jnp.einsum(
        "shwd,wkc->shkcd", tokens, column_forward, preferred_element_type=jnp.float32
    ).astype(jnp.bfloat16)
    spectrum = along_rows(lax.all_to_all(spec_rows, "seq", split_axis=2, concat_axis=1, tiled=True))
    flat_modes, hidden_pre, hidden, spectrum_out = mix_forward(
        spectrum, weights_in, weights_out, bias_in, bias_out
    )
    mixed_grid = jnp.einsum(
        "shkcd,kcw->shwd",
        lax.all_to_all(back_rows(spectrum_out), "seq", split_axis=1, concat_axis=2, tiled=True),
        column_inverse,
        preferred_element_type=jnp.float32,
    )
    cot_rows = jnp.einsum(
        "shwd,kcw->shkcd", cotangent, column_inverse, preferred_element_type=jnp.float32
    ).astype(jnp.bfloat16)
    incoming = along_rows(lax.all_to_all(cot_rows, "seq", split_axis=2, concat_axis=1, tiled=True))
    spectrum_grad, partials = mix_backward(
        flat_modes, hidden_pre, hidden, incoming, weights_in, weights_out
    )
    adjoint_part = jnp.einsum(
        "shkcd,wkc->shwd",
        lax.all_to_all(back_rows(spectrum_grad), "seq", split_axis=1, concat_axis=2, tiled=True),
        column_forward,
        preferred_element_type=jnp.float32,
    )
    mixed_out = (tokens.astype(jnp.float32) + mixed_grid).astype(jnp.bfloat16)
    tokens_grad = (cotangent.astype(jnp.float32) + adjoint_part).astype(jnp.bfloat16)
    totals = lax.psum((partials[0], partials[1], partials[2], partials[3]), ("seq", "rep"))
    divisor = float(samples * lax.axis_size("rep"))
    return (
        mixed_out,
        tokens_grad,
        totals[0] / divisor,
        totals[1] / divisor,
        totals[2] / divisor,
        totals[3] / divisor,
    )


GROUP = math.lcm(BLOCK, 128)
PER_GROUP = GROUP // BLOCK
MESH_ID = pl.DeviceIdType.MESH
VMEM_LIMIT = 52 << 20
FIRST, AFTER_E, AFTER_F = 2, 3, 2
SPREAD = 11
GREET = 9


def host_tables(length, modes):
    residue = np.arange(length)[:, None] * np.arange(modes)[None, :] % length
    angles = residue.astype(np.float32) * np.float32(2.0 * math.pi / length)
    factor = np.float32(1.0 / math.sqrt(length))
    rounded = [(f(angles) * factor).astype(ml_dtypes.bfloat16) for f in (np.cos, np.sin)]
    return [table.astype(np.float32) for table in rounded]


def kernel_tables(width, length, n, samples, rows):
    local = MODES // n
    cosine, sine = host_tables(width, MODES)
    forward = np.stack([cosine.T, -sine.T], axis=1)
    doubled = forward * np.where(np.arange(MODES) == 0, 1.0, 2.0)[:, None, None]

    def spread(table):
        table = table.reshape(n, local, 2, width)
        whole = np.zeros((n, samples, local, 2, width, samples), np.float32)
        for s in range(samples):
            whole[:, s, :, :, :, s] = table
        return whole.reshape(n * samples * local * 2, width * samples)

    cosine, sine = host_tables(length, length)
    upper = np.stack([cosine, sine], axis=2)
    lower = np.stack([-sine, cosine], axis=2)
    turn = np.stack([upper, lower], axis=0)
    both = samples * local
    mixing = np.zeros((2, both, length, length, both, 2), np.float32)
    for x in range(both):
        mixing[:, x, :, :, x, :] = turn
    mixing = mixing.reshape(2 * both * length, length * both * 2)

    flat = [
        spread(forward),
        spread(doubled),
        spread(doubled).T,
        spread(forward).T,
        mixing,
    ]
    return [np.ascontiguousarray(t).astype(ml_dtypes.bfloat16) for t in flat]


def dot(a, b, contract=(1, 0)):
    return lax.dot_general(
        a, b, (((contract[0],), (contract[1],)), ((), ())), preferred_element_type=jnp.float32
    )


def mixer(
    n,
    inner,
    divisor,
    tok_far,
    cot_far,
    col_tok_far,
    col_cot_far,
    inv_mix_far,
    inv_grad_far,
    turn_far,
    in_weight_far,
    in_bias_far,
    out_weight_far,
    out_bias_far,
    mixed,
    grad,
    in_weight_grad,
    in_bias_grad,
    out_weight_grad,
    out_bias_grad,
    tok,
    cot,
    col_tok,
    col_cot,
    inv_mix,
    inv_grad,
    turn,
    in_weight,
    in_bias,
    out_weight,
    out_bias,
    send_a,
    send_b,
    send_c,
    send_d,
    recv_a,
    recv_b,
    recv_c,
    recv_d,
    send_e,
    send_f,
    recv_e,
    recv_f,
    turn_back,
    wide,
    spec,
    hid,
    slope,
    inc,
    pre,
    mixed_modes,
    grads,
    halves,
    half_in,
    gathered,
    other,
    both,
    send_sem,
    recv_sem,
    pair_send,
    pair_recv,
    load_sem,
):
    me = lax.axis_index("seq")
    core = lax.axis_index("rep")
    partner = 1 - core
    rows, width, samples, channels = tok.shape
    groups = channels // GROUP
    outer = n // inner
    across, within = me // inner, lax.rem(me, inner)
    chunk = send_a.shape[2]
    row_chunk = chunk // rows
    bf16 = jnp.bfloat16

    barrier = pltpu.get_barrier_semaphore()

    def greet(j, carry):
        peer = lax.rem(me + j * GREET, n)
        pl.semaphore_signal(barrier, inc=1, device_id={"seq": peer}, device_id_type=MESH_ID)
        return carry

    lax.fori_loop(1, n, greet, 0)
    pl.semaphore_signal(barrier, inc=1, device_id={"rep": partner}, device_id_type=MESH_ID)

    moves = [(col_tok_far, col_tok)]
    moves += [(tok_far.at[h], tok.at[h]) for h in range(rows)]
    moves += [(col_cot_far, col_cot)]
    moves += [(cot_far.at[h], cot.at[h]) for h in range(rows)]
    moves += [
        (in_weight_far, in_weight),
        (out_weight_far, out_weight),
        (turn_far, turn),
        (in_bias_far, in_bias),
        (out_bias_far, out_bias),
        (inv_mix_far, inv_mix),
        (inv_grad_far, inv_grad),
    ]
    loads = [
        pltpu.make_async_copy(far, near, load_sem.at[i]) for i, (far, near) in enumerate(moves)
    ]
    for load in loads[: rows + 1]:
        load.start()

    def copy_to(slot, peer, source, target):
        return pltpu.make_async_remote_copy(
            src_ref=source,
            dst_ref=target,
            send_sem=send_sem.at[slot],
            recv_sem=recv_sem.at[slot],
            device_id={"seq": peer},
            device_id_type=MESH_ID,
        )

    def loop(count, act):
        def step(j, carry):
            act(j)
            return carry

        lax.fori_loop(1, count, step, 0)

    def peer_at(j):
        peer = jnp.int32(0)
        j = lax.rem(j * SPREAD, n)
        bit = 1
        while bit < n:
            peer = peer + bit * lax.rem(me // bit + j // bit, 2)
            bit *= 2
        return peer

    class Move:
        def __init__(self, slot, count, to, source, target, span):
            self.slot, self.count, self.to = slot, count, to
            self.source, self.target, self.span = source, target, span

        def start(self):
            def out(j):
                at, peer = self.to(j)
                copy_to(self.slot, peer, self.source(at), self.target).start()

            loop(self.count, out)

        def all(self):
            return copy_to(self.slot, me, self.span, self.span)

        def arrived(self):
            self.all().wait_recv()

        def left(self):
            self.all().wait_send()

    def to_peer(j):
        peer = peer_at(j)
        return peer, peer

    def to_plane(j):
        v = lax.rem(within + j, inner)
        return v, across * inner + v

    def everyone(slot, source, target, g, at=None):
        cut = pl.ds(0, chunk) if at is None else at
        return Move(
            slot,
            n,
            to_peer,
            lambda peer: source.at[g, peer, cut],
            target.at[g, me, cut],
            target.at[g, pl.ds(0, n - 1), cut],
        )

    def move_a(g):
        return everyone(g, send_a, recv_a, g)

    def move_b(g):
        return everyone(groups + g, send_b, recv_b, g)

    def move_c(g, h):
        at = pl.ds(h * row_chunk, row_chunk)
        return everyone(2 * groups + g * rows + h, send_c, recv_c, g, at)

    def move_d(g, h):
        at = pl.ds(h * row_chunk, row_chunk)
        return everyone((2 + rows) * groups + g * rows + h, send_d, recv_d, g, at)

    tail = (2 + 2 * rows) * groups
    move_e = Move(
        tail,
        inner,
        to_plane,
        lambda v: send_e.at[v],
        recv_e.at[within],
        recv_e.at[pl.ds(0, inner - 1)],
    )
    move_f = copy_to(tail + 1, (1 - across) * inner + within, send_f, recv_f)
    move_g = Move(
        tail + 2,
        inner,
        to_plane,
        lambda v: gathered.at[within],
        gathered.at[within],
        gathered.at[pl.ds(0, inner - 1)],
    )

    def lanes(g):
        return pl.ds(pl.multiple_of(g * GROUP, GROUP), GROUP)

    def fixed(g):
        return pl.ds(g * GROUP, GROUP)

    def columns(tokens, table, send, g):
        for h in range(rows):
            section = tokens[h, :, :, fixed(g)].reshape(width * samples, GROUP)
            send[g, :, h * row_chunk : (h + 1) * row_chunk, :] = (
                dot(table[...], section).astype(bf16).reshape(n, row_chunk, GROUP)
            )

    for load in loads[: rows + 1]:
        load.wait()
    for load in loads[rows + 1 :]:
        load.start()
    for g in range(groups):
        columns(tok, col_tok, send_a, g)
        if g == 0:
            pl.semaphore_wait(barrier, n)
        move_a(g).start()
        if g == 0:
            for load in loads[rows + 1 : 2 * rows + 2]:
                load.wait()
        columns(cot, col_cot, send_b, g)
        move_b(g).start()
    for load in loads[2 * rows + 2 :]:
        load.wait()
    recv_a[:, me] = send_a[:, me]
    recv_b[:, me] = send_b[:, me]

    turn_back[...] = turn[...].T
    row_at = lax.broadcasted_iota(jnp.int32, (BLOCK, GROUP), 0)
    lane_at = lax.broadcasted_iota(jnp.int32, (BLOCK, GROUP), 1)
    for at, weight in enumerate((in_weight, out_weight)):
        for i in range(PER_GROUP):
            place = (lane_at == row_at + i * BLOCK).astype(bf16)
            for c in range(2):
                for g in range(groups):
                    wide[2 * at + c, g, i * BLOCK : (i + 1) * BLOCK, :] = dot(
                        weight[c, g * PER_GROUP + i], place
                    ).astype(bf16)

    half = turn.shape[0] // 2
    scale = math.sqrt(2.0 / math.pi)

    def per_group(act):
        def step(g, carry):
            act(g, lanes(g))
            return carry

        lax.fori_loop(0, groups, step, 0)

    def along_rows(recv, keep, g):
        keep[g] = dot(turn[...], recv[g].reshape(turn.shape[1], GROUP)).astype(bf16)

    def back_rows(send, g):
        send[g] = dot(turn_back[...], mixed_modes[...]).astype(bf16).reshape(n, chunk, GROUP)

    def forward_group(g, at):
        along_rows(recv_a, spec, g)
        re, im = spec[g, :half], spec[g, half:]
        w_re, w_im = wide[0, g], wide[1, g]
        for c in range(2):
            if c == 0:
                value = dot(re, w_re) - dot(im, w_im)
            else:
                value = dot(re, w_im) + dot(im, w_re)
            value = value + in_bias[c : c + 1, at]
            square = value * value
            tanh = jnp.tanh(scale * value * (1.0 + 0.044715 * square))
            hid[g, c * half : (c + 1) * half] = (0.5 * value * (1.0 + tanh)).astype(bf16)
            slope[g, c * half : (c + 1) * half] = 0.5 * (1.0 + tanh) + 0.5 * value * (
                1.0 - tanh * tanh
            ) * (scale * (1.0 + (3.0 * 0.044715) * square))
        re, im = hid[g, :half], hid[g, half:]
        w_re, w_im = wide[2, g], wide[3, g]
        mixed_modes[:half] = (
            dot(re, w_re) - dot(im, w_im) + out_bias[0:1, at]
        ).astype(bf16)
        mixed_modes[half:] = (
            dot(re, w_im) + dot(im, w_re) + out_bias[1:2, at]
        ).astype(bf16)
        back_rows(send_c, g)

    def backward_group(g):
        along_rows(recv_b, inc, g)
        re, im = inc[g, :half], inc[g, half:]
        w_re, w_im = wide[2, g], wide[3, g]
        pre[g, :half] = (
            (dot(re, w_re, (1, 1)) + dot(im, w_im, (1, 1))) * slope[g, :half]
        ).astype(bf16)
        pre[g, half:] = (
            (dot(im, w_re, (1, 1)) - dot(re, w_im, (1, 1))) * slope[g, half:]
        ).astype(bf16)
        re, im = pre[g, :half], pre[g, half:]
        w_re, w_im = wide[0, g], wide[1, g]
        mixed_modes[:half] = (dot(re, w_re, (1, 1)) + dot(im, w_im, (1, 1))).astype(bf16)
        mixed_modes[half:] = (dot(im, w_re, (1, 1)) - dot(re, w_im, (1, 1))).astype(bf16)
        back_rows(send_d, g)

    def fold(product):
        total = jnp.zeros((BLOCK, GROUP), jnp.float32)
        for i in range(PER_GROUP):
            inside = (lane_at >= i * BLOCK) & (lane_at < (i + 1) * BLOCK)
            total = jnp.where(inside, product[i * BLOCK : (i + 1) * BLOCK], total)
        return total.astype(bf16)

    bias_at = lax.broadcasted_iota(jnp.int32, (16, GROUP), 0)

    def grads_group(g, at):
        bias = jnp.zeros((16, GROUP), jnp.float32)
        for k, (left, right) in enumerate(((spec, pre), (hid, inc))):
            a_re, a_im = left[g, :half], left[g, half:]
            b_re, b_im = right[g, :half], right[g, half:]
            first = 2 * k * BLOCK
            grads[first : first + BLOCK, at] = fold(
                dot(a_re, b_re, (0, 0)) + dot(a_im, b_im, (0, 0))
            )
            grads[first + BLOCK : first + 2 * BLOCK, at] = fold(
                dot(a_re, b_im, (0, 0)) - dot(a_im, b_re, (0, 0))
            )
            for c, value in enumerate((b_re, b_im)):
                total = jnp.sum(value.astype(jnp.float32), axis=0, keepdims=True)
                bias = jnp.where(bias_at == 2 * k + c, total, bias)
        grads[4 * BLOCK : 4 * BLOCK + 16, at] = bias.astype(bf16)

    last = groups - 1
    held = [move_c(last, h) for h in range(rows)]
    held += [move_d(g, h) for g in range(groups) for h in range(rows)]

    def release(count):
        for move in held[:count]:
            move.start()
        del held[:count]

    def mix_group(g, at):
        with jax.named_scope("wait_a"):
            move_a(g).arrived()
        with jax.named_scope("fwd"):
            forward_group(g, at)
        recv_c[g, me] = send_c[g, me]

        @pl.when(g < last)
        def _():
            for h in range(rows):
                move_c(g, h).start()

        with jax.named_scope("wait_b"):
            move_b(g).arrived()

        @pl.when(g == last)
        def _():
            release(FIRST)

        with jax.named_scope("bwd"):
            backward_group(g)
        recv_d[g, me] = send_d[g, me]
        with jax.named_scope("grads"):
            grads_group(g, at)

    per_group(mix_group)

    per = 4 * BLOCK // (2 * n)
    to_row = lax.broadcasted_iota(jnp.int32, (2 * n * 16, 4 * BLOCK + 16), 0)
    from_row = lax.broadcasted_iota(jnp.int32, (2 * n * 16, 4 * BLOCK + 16), 1)
    slot = to_row % 16
    wanted = jnp.where(slot < per, to_row // 16 * per + slot, 4 * BLOCK + slot - per)
    picks = (wanted == from_row).astype(bf16)
    halves[...] = dot(picks, grads[...]).astype(bf16).reshape(halves.shape)

    def swap(slot, source, target):
        return pltpu.make_async_remote_copy(
            src_ref=source,
            dst_ref=target,
            send_sem=pair_send.at[slot],
            recv_sem=pair_recv.at[slot],
            device_id={"rep": partner},
            device_id_type=MESH_ID,
        )

    first_swap = swap(0, halves.at[partner], half_in)
    first_swap.start()

    def inverse_row(h, g, tokens, table, recv, out):
        section = recv[g, :, h * row_chunk : (h + 1) * row_chunk, :]
        product = dot(table[...], section.reshape(n * row_chunk, GROUP))
        kept = tokens[h, :, :, fixed(g)].reshape(width * samples, GROUP).astype(jnp.float32)
        out[h, :, :, fixed(g)] = (kept + product).astype(bf16).reshape(width, samples, GROUP)

    with jax.named_scope("swap1"):
        first_swap.wait()
    send_e[...] = (
        (halves[core].astype(jnp.float32) + half_in[...].astype(jnp.float32))
        .astype(bf16)
        .reshape(send_e.shape)
    )
    move_e.start()
    recv_e[within] = send_e[within]
    release(AFTER_E)
    with jax.named_scope("wait_e"):
        move_e.arrived()
    send_f[...] = jnp.sum(recv_e[...].astype(jnp.float32), axis=0).astype(bf16)
    move_f.start()
    release(AFTER_F)
    with jax.named_scope("wait_f"):
        move_f.wait_recv()
    total = (send_f[...].astype(jnp.float32) + recv_f[...].astype(jnp.float32)) * (1.0 / divisor)
    in_bias_grad[...] = total[0, per : per + 2]
    out_bias_grad[...] = total[0, per + 2 : per + 4]
    gathered[within] = total.astype(bf16)
    move_g.start()
    release(len(held))
    def finish_c(g, h):
        with jax.named_scope(f"wait_c{g}{h}"):
            move_c(g, h).arrived()
        inverse_row(h, g, tok, inv_mix, recv_c, mixed)

    def finish_d(g, h):
        with jax.named_scope(f"wait_d{g}{h}"):
            move_d(g, h).arrived()
        inverse_row(h, g, cot, inv_grad, recv_d, grad)

    for g in range(groups):
        for h in range(rows):
            finish_c(g, h)
    for g in range(groups):
        move_a(g).left()
        move_b(g).left()
    move_e.left()
    move_f.wait_send()
    for g in range(last):
        for h in range(rows):
            finish_d(g, h)
    with jax.named_scope("wait_g"):
        move_g.arrived()
    last_swap = swap(1, gathered, other)
    last_swap.start()
    both[core] = gathered[...].reshape(n * 16, channels)
    move_g.left()
    for g in range(groups):
        for h in range(rows):
            move_c(g, h).left()
    finish_d(last, 0)
    with jax.named_scope("swap2"):
        last_swap.wait()
    both[partner] = other[...].reshape(n * 16, channels)
    to_row = lax.broadcasted_iota(jnp.int32, (2 * BLOCK, n * 16), 0)
    from_row = lax.broadcasted_iota(jnp.int32, (2 * BLOCK, n * 16), 1)
    order = (to_row // per * 16 + to_row % per == from_row).astype(bf16)
    with jax.named_scope("params"):
        for k, out in enumerate((in_weight_grad, out_weight_grad)):
            for g in range(groups):
                ordered = dot(order, both[k, :, g * GROUP : (g + 1) * GROUP]).astype(bf16)
                for i in range(PER_GROUP):
                    place = (lane_at == row_at + i * BLOCK).astype(bf16)
                    block = dot(ordered, place, (1, 1))
                    for c in range(2):
                        out[c, g * PER_GROUP + i] = block[c * BLOCK : (c + 1) * BLOCK]
    for h in range(1, rows - 1):
        finish_d(last, h)
    for g in range(last):
        for h in range(rows):
            move_d(g, h).left()
    for h in range(rows - 1):
        move_d(last, h).left()
    finish_d(last, rows - 1)
    with jax.named_scope("end"):
        move_d(last, rows - 1).left()


def settle(*refs):
    count = len(refs) // 2
    near, far, sems = refs[:count], refs[count:-1], refs[-1]
    copies = [
        pltpu.make_async_copy(a, b, sems.at[i]) for i, (a, b) in enumerate(zip(near, far))
    ]
    for copy in copies:
        copy.start()
    for copy in copies:
        copy.wait()


def fits(n, reps, samples, rows, channels):
    per_row = samples * (MODES // n) * 2
    return (
        reps == 2
        and MODES % n == 0
        and per_row % 16 == 0
        and channels % GROUP == 0
        and channels == BLOCKS * BLOCK
        and (4 * BLOCK) % (2 * n) == 0
        and n > 3
        and n & (n - 1) == 0
        and rows > 1
        and 4 * BLOCK // (2 * n) + 4 <= 16
        and (samples * MODES // n * rows * n) % 16 == 0
    )


def shards(tokens, cotangent, in_weight, in_bias, out_weight, out_bias):
    samples, rows, width, channels = tokens.shape
    n, reps = lax.axis_size("seq"), lax.axis_size("rep")
    if not fits(n, reps, samples, rows, channels):
        return shards_plain(tokens, cotangent, in_weight, in_bias, out_weight, out_bias)
    length = rows * n
    outer = 2
    inner = n // outer
    chunk = rows * samples * (MODES // n) * 2
    whole = n * chunk
    groups = channels // GROUP
    tables = [jnp.asarray(t) for t in kernel_tables(width, length, n, samples, rows)]
    bf16, f32 = jnp.bfloat16, jnp.float32
    block = pltpu.VMEM((groups, n, chunk, GROUP), bf16)
    small = pltpu.VMEM((n, 16, channels), bf16)
    ringed = pltpu.VMEM((inner, outer, 16, channels), bf16)
    lined = pltpu.VMEM((outer, 16, channels), bf16)
    planes = (tokens.transpose(1, 2, 0, 3), cotangent.transpose(1, 2, 0, 3))
    kept = pltpu.VMEM((groups, whole, GROUP), bf16)
    anywhere = pl.BlockSpec(memory_space=pl.ANY)
    far = pl.BlockSpec(memory_space=pltpu.HBM)
    inputs = (*planes, *tables, in_weight, in_bias, out_weight, out_bias)
    shapes = (
        (planes[0].shape, bf16),
        (planes[1].shape, bf16),
        (in_weight.shape, f32),
        (in_bias.shape, f32),
        (out_weight.shape, f32),
        (out_bias.shape, f32),
    )
    near = pl.pallas_call(
        functools.partial(mixer, n, inner, float(samples * reps)),
        out_shape=tuple(pltpu.VMEM(*shape) for shape in shapes),
        in_specs=[far] * 11,
        grid=(1,),
        out_specs=(pl.BlockSpec(memory_space=pltpu.VMEM),) * 6,
        scratch_shapes=[pltpu.VMEM(v.shape, v.dtype) for v in inputs]
        + [block] * 8
        + [ringed, lined] * 2
        + [
            pltpu.VMEM((whole, whole), bf16),
            pltpu.VMEM((4, groups, GROUP, GROUP), bf16),
            kept,
            kept,
            pltpu.VMEM((groups, whole, GROUP), f32),
            kept,
            kept,
            pltpu.VMEM((whole, GROUP), bf16),
            pltpu.VMEM((4 * BLOCK + 16, channels), bf16),
            pltpu.VMEM((2, n, 16, channels), bf16),
            small,
            ringed,
            ringed,
            pltpu.VMEM((2, n * 16, channels), bf16),
            pltpu.SemaphoreType.DMA(((2 + 2 * rows) * groups + 3,)),
            pltpu.SemaphoreType.DMA(((2 + 2 * rows) * groups + 3,)),
            pltpu.SemaphoreType.DMA((2,)),
            pltpu.SemaphoreType.DMA((2,)),
            pltpu.SemaphoreType.DMA((2 * rows + 9,)),
        ],
        compiler_params=pltpu.CompilerParams(
            collective_id=0, has_side_effects=True, vmem_limit_bytes=VMEM_LIMIT
        ),
        name="mixer",
    )(*inputs)
    mixed, grad, *parameter_grads = pl.pallas_call(
        settle,
        out_shape=tuple(jax.ShapeDtypeStruct(*shape) for shape in shapes),
        in_specs=[anywhere] * 6,
        out_specs=(far,) * 6,
        scratch_shapes=[pltpu.SemaphoreType.DMA((6,))],
        compiler_params=pltpu.CompilerParams(vmem_limit_bytes=1 << 20),
        name="settle",
    )(*(pltpu.with_memory_space_constraint(part, pltpu.VMEM) for part in near))
    return (
        mixed.transpose(2, 0, 1, 3),
        grad.transpose(2, 0, 1, 3),
        *parameter_grads,
    )


def solution(mesh):
    in_specs = (P("rep", "seq", None, None), P("rep", "seq", None, None), P(), P(), P(), P())
    out_specs = (P("rep", "seq", None, None), P("rep", "seq", None, None), P(), P(), P(), P())
    return jax.shard_map(shards, mesh=mesh, in_specs=in_specs, out_specs=out_specs, check_vma=False)
```
